16 devices in a mesh: dp: 4 (over z, y), ep: 4 (over x, core).
Axes of the slice: x: 2, y: 2, z: 2, core: 2. Of those that a mesh axis runs over, the one named last changes fastest.
Arguments:
- h0: bfloat16 [16, 256, 2048], P(('dp', 'ep')), parts along dimension 0
- idx: int32 [16, 256, 6], P(('dp', 'ep')), parts along dimension 0
- slot: int32 [16, 256, 6], P(('dp', 'ep')), parts along dimension 0
- ln_attn: bfloat16 [2048], replicated
- wq: bfloat16 [2048, 2048], replicated
- wk: bfloat16 [2048, 2048], replicated
- wv: bfloat16 [2048, 2048], replicated
- wo: bfloat16 [2048, 2048], replicated
- ln_ffn: bfloat16 [2048], replicated
- ws1: bfloat16 [2048, 2816], replicated
- ws3: bfloat16 [2048, 2816], replicated
- ws2: bfloat16 [2816, 2048], replicated
- ln_moe: bfloat16 [2048], replicated
- wr: bfloat16 [2048, 64], replicated
- ue1: bfloat16 [64, 2048, 1408], P('ep')
- ue3: bfloat16 [64, 2048, 1408], P('ep')
- ue2: bfloat16 [64, 1408, 2048], P('ep')
Outputs:
- output: bfloat16 [16, 256, 2048], P(('dp', 'ep')), parts along dimension 0
There are 4 independent parts. The reference program is written for one: setup_inputs(seed, part) draws one part's arguments, and reference() takes and returns one part's arrays. A program takes and returns all parts, laid end to end along the dimension named above; an argument that names none is the same for every part.
All inputs are finite; a program needn't handle non-finite values.
Results may differ from the reference program's by a relative error of at most 0.00929055.
Values are sent between devices in bfloat16 or wider.
A program may use at most 1.5 GiB of HBM per device.

```python
import jax
import jax.numpy as jnp
from jax import lax

D = 2048
HEADS = 16
HEAD = 128
EXPERTS = 64
TOP = 6
FE = 1408
FS = 2816
SEQ = 256
SEQS = 1
G = 4
CAP = 48

T = SEQS * SEQ
EPS = 1e-6


def _dot(a, b):
    return jnp.dot(a, b, preferred_element_type=jnp.float32)


def _rms(x, w):
    xf = x.astype(jnp.float32)
    r = lax.rsqrt(jnp.mean(xf * xf, axis=-1, keepdims=True) + EPS)
    return (xf * r * w.astype(jnp.float32)).astype(jnp.bfloat16)


def _rope(x):
    half = HEAD // 2
    freq = 10000.0 ** (-jnp.arange(half, dtype=jnp.float32) / half)
    ang = jnp.arange(SEQ, dtype=jnp.float32)[:, None] * freq[None, :]
    c = jnp.cos(ang)[:, None, :]
    s = jnp.sin(ang)[:, None, :]
    x1, x2 = x[..., :half], x[..., half:]
    return jnp.concatenate([x1 * c - x2 * s, x2 * c + x1 * s], axis=-1)


def _normal(key, shape, scale):
    return (jax.random.normal(key, shape, jnp.float32) * scale).astype(jnp.bfloat16)


def _scale(key):
    return jax.random.uniform(key, (D,), jnp.float32, 0.8, 1.2).astype(jnp.bfloat16)


def _expert_weight(weight_key):
    levels = jnp.sum(jax.random.randint(weight_key, (9, EXPERTS), 0, 10, jnp.int32), axis=0)
    hot_bias = 12 * (jnp.arange(EXPERTS) < EXPERTS // G).astype(jnp.int32)
    quarter = jnp.maximum(levels + hot_bias - 16, 0)
    return jnp.left_shift(4 + quarter % 4, quarter // 4).astype(jnp.int32)


def _route(route_key, weight):
    draw_rows = jax.random.bits(route_key, (T, TOP), jnp.uint32)

    def step(counts, draw_row):
        open_weight = jnp.where(counts < CAP, weight, 0).astype(jnp.int32)
        picked_list = []
        for choice in range(TOP):
            cumulative = jnp.cumsum(open_weight)
            total_weight = cumulative[-1].astype(jnp.uint32)
            target_val = (draw_row[choice] % total_weight).astype(jnp.int32)
            pick_id = jnp.searchsorted(cumulative, target_val, side='right').astype(jnp.int32)
            picked_list.append(pick_id)
            open_weight = open_weight.at[pick_id].set(0)
        chosen = jnp.stack(picked_list)
        return counts.at[chosen].add(1), (chosen, counts[chosen])

    _, (chosen, slots) = lax.scan(step, jnp.zeros((EXPERTS,), jnp.int32), draw_rows)
    return chosen.astype(jnp.int32), slots.astype(jnp.int32)


def setup_inputs(seed: int = 0, part: int = 0) -> dict:
    key = jax.random.PRNGKey(seed)
    kh, kr = jax.random.split(jax.random.fold_in(key, part))
    ks = jax.random.split(key, 15)
    hd = HEADS * HEAD
    expert_weight = _expert_weight(jax.random.fold_in(ks[14], 7))
    idx, slot = jax.vmap(lambda k: _route(k, expert_weight))(jax.random.split(kr, G))
    return {
        'h0': _normal(kh, (G * SEQS, SEQ, D), 1.0),
        'idx': idx.reshape(G * SEQS, SEQ, TOP),
        'slot': slot.reshape(G * SEQS, SEQ, TOP),
        'ln_attn': _scale(ks[0]),
        'wq': _normal(ks[1], (D, hd), 1.5 * D ** -0.5),
        'wk': _normal(ks[2], (D, hd), 1.5 * D ** -0.5),
        'wv': _normal(ks[3], (D, hd), D ** -0.5),
        'wo': _normal(ks[4], (hd, D), hd ** -0.5),
        'ln_ffn': _scale(ks[5]),
        'ws1': _normal(ks[6], (D, FS), D ** -0.5),
        'ws3': _normal(ks[7], (D, FS), D ** -0.5),
        'ws2': _normal(ks[8], (FS, D), FS ** -0.5),
        'ln_moe': _scale(ks[9]),
        'wr': _normal(ks[10], (D, EXPERTS), 1.5 * D ** -0.5),
        'ue1': _normal(ks[11], (EXPERTS, D, FE), D ** -0.5),
        'ue3': _normal(ks[12], (EXPERTS, D, FE), D ** -0.5),
        'ue2': _normal(ks[13], (EXPERTS, FE, D), 2.0 * FE ** -0.5),
    }


def reference(h0, idx, slot, ln_attn, wq, wk, wv, wo, ln_ffn, ws1, ws3, ws2, ln_moe, wr, ue1, ue3, ue2):
    nb = h0.shape[0]
    n = nb * SEQ
    x1 = _rms(h0, ln_attn)
    causal = jnp.arange(SEQ)[:, None] >= jnp.arange(SEQ)[None, :]

    def attn(xs):
        q = _rope(_dot(xs, wq).reshape(SEQ, HEADS, HEAD)).astype(jnp.bfloat16)
        k = _rope(_dot(xs, wk).reshape(SEQ, HEADS, HEAD)).astype(jnp.bfloat16)
        v = _dot(xs, wv).astype(jnp.bfloat16).reshape(SEQ, HEADS, HEAD)
        s = jnp.einsum('qhe,khe->hqk', q.astype(jnp.float32), k.astype(jnp.float32)) * HEAD ** -0.5
        p = jax.nn.softmax(jnp.where(causal[None], s, -1e30), axis=-1).astype(jnp.bfloat16)
        o = jnp.einsum('hqk,khe->qhe', p.astype(jnp.float32), v.astype(jnp.float32))
        return o.astype(jnp.bfloat16).reshape(SEQ, HEADS * HEAD)

    o = lax.map(attn, x1).reshape(n, HEADS * HEAD)
    h = h0.reshape(n, D)
    a = (h.astype(jnp.float32) + _dot(o, wo)).astype(jnp.bfloat16)
    x2 = _rms(a, ln_ffn)
    hs = (jax.nn.silu(_dot(x2, ws1)) * _dot(x2, ws3)).astype(jnp.bfloat16)
    f = _dot(hs, ws2)

    u = _rms(h, ln_moe)
    gi = idx.reshape(n, TOP)
    sl = slot.reshape(n, TOP)
    g = jax.nn.softmax(jnp.take_along_axis(_dot(u, wr), gi, axis=1), axis=-1)
    dev = jnp.arange(n, dtype=jnp.int32) // T
    pos = gi * (G * CAP) + dev[:, None] * CAP + sl
    src = jnp.full((EXPERTS * G * CAP,), n, jnp.int32).at[pos.reshape(-1)].set(
        jnp.arange(n * TOP, dtype=jnp.int32) // TOP)
    u_pad = jnp.concatenate([u, jnp.zeros((1, D), jnp.bfloat16)], axis=0)
    buf = u_pad[src].reshape(EXPERTS, G * CAP, D)

    def expert(args):
        x, w1, w3, w2 = args
        he = (jax.nn.silu(_dot(x, w1)) * _dot(x, w3)).astype(jnp.bfloat16)
        return _dot(he, w2).astype(jnp.bfloat16)

    y = lax.map(expert, (buf, ue1, ue3, ue2)).reshape(EXPERTS * G * CAP, D)
    m = jnp.sum(g[:, :, None] * y[pos].astype(jnp.float32), axis=1)
    out = a.astype(jnp.float32) + f + m
    return out.astype(jnp.bfloat16).reshape(nb, SEQ, D)
```

```python
import jax
import jax.numpy as jnp
from jax import lax
from jax.sharding import PartitionSpec as P

HEAD = 128
EPS = 1e-6
CAP_FACTOR = 2


def _mm(form, a, b):
    return jnp.einsum(form, a, b, preferred_element_type=jnp.float32)


def _rms(x, w):
    xf = x.astype(jnp.float32)
    r = lax.rsqrt(jnp.mean(xf * xf, axis=-1, keepdims=True) + EPS)
    return (xf * r * w.astype(jnp.float32)).astype(jnp.bfloat16)


def _rope(x):
    s, half = x.shape[1], x.shape[-1] // 2
    freq = 10000.0 ** (-jnp.arange(half, dtype=jnp.float32) / half)
    ang = jnp.arange(s, dtype=jnp.float32)[:, None] * freq[None, :]
    c = jnp.cos(ang)[None, :, None, :]
    sn = jnp.sin(ang)[None, :, None, :]
    x1, x2 = x[..., :half], x[..., half:]
    return jnp.concatenate([x1 * c - x2 * sn, x2 * c + x1 * sn], axis=-1)


def _dense(h0, ln_attn, wq, wk, wv, wo, ln_ffn, ws1, ws3, ws2):
    b, s, _ = h0.shape
    nh = wq.shape[1] // HEAD
    x1 = _rms(h0, ln_attn)
    q = _rope(_mm('bsd,de->bse', x1, wq).reshape(b, s, nh, HEAD)).astype(jnp.bfloat16)
    k = _rope(_mm('bsd,de->bse', x1, wk).reshape(b, s, nh, HEAD)).astype(jnp.bfloat16)
    v = _mm('bsd,de->bse', x1, wv).astype(jnp.bfloat16).reshape(b, s, nh, HEAD)
    sc = _mm('bqhe,bkhe->bhqk', q, k) * HEAD ** -0.5
    causal = jnp.arange(s)[:, None] >= jnp.arange(s)[None, :]
    p = jax.nn.softmax(jnp.where(causal, sc, -1e30), axis=-1).astype(jnp.bfloat16)
    o = _mm('bhqk,bkhe->bqhe', p, v).astype(jnp.bfloat16).reshape(b, s, nh * HEAD)
    a = (h0.astype(jnp.float32) + _mm('bse,ed->bsd', o, wo)).astype(jnp.bfloat16)
    x2 = _rms(a, ln_ffn)
    hs = (jax.nn.silu(_mm('bsd,df->bsf', x2, ws1)) * _mm('bsd,df->bsf', x2, ws3)).astype(jnp.bfloat16)
    return a, _mm('bsf,fd->bsd', hs, ws2)


def _experts(x, ue1, ue3, ue2):
    he = (jax.nn.silu(_mm('gecd,edf->egcf', x, ue1)) * _mm('gecd,edf->egcf', x, ue3)).astype(jnp.bfloat16)
    return _mm('egcf,efd->gecd', he, ue2).astype(jnp.bfloat16)


def _gate(u, wr, gi):
    lg = _mm('td,de->te', u, wr)
    hit = gi[..., None] == jnp.arange(wr.shape[1], dtype=gi.dtype)
    return jax.nn.softmax(jnp.sum(jnp.where(hit, lg[:, None, :], 0.0), axis=-1), axis=-1)


def _parts(c):
    hi = c.astype(jnp.bfloat16)
    r = c - hi.astype(jnp.float32)
    mid = r.astype(jnp.bfloat16)
    lo = (r - mid.astype(jnp.float32)).astype(jnp.bfloat16)
    return hi, mid, lo


def solution(mesh):
    rows = P(('dp', 'ep'))
    rep = P()
    core = [(k, k ^ 1) for k in range(4)]
    chip = [(k, k ^ 2) for k in range(4)]

    def local(h0, idx, slot, ln_attn, wq, wk, wv, wo, ln_ffn, ws1, ws3, ws2, ln_moe, wr, ue1, ue3, ue2):
        b, s, d = h0.shape
        top = idx.shape[-1]
        el = ue1.shape[0]
        t = b * s
        cap = CAP_FACTOR * t * top // (el * mesh.shape['ep'])
        u = _rms(h0, ln_moe).reshape(t, d)
        gi = idx.reshape(t, top)
        gate = _gate(u, wr, gi)
        pos = (gi * cap + slot.reshape(t, top)).astype(jnp.float32)
        pk = jnp.concatenate([pos, gate], axis=-1)
        ux, kx = lax.ppermute(u, 'ep', chip), lax.ppermute(pk, 'ep', chip)
        uc, kc = lax.ppermute(u, 'ep', core), lax.ppermute(pk, 'ep', core)
        uxc, kxc = lax.ppermute(ux, 'ep', core), lax.ppermute(kx, 'ep', core)
        a, fo = _dense(h0, ln_attn, wq, wk, wv, wo, ln_ffn, ws1, ws3, ws2)
        us = jnp.stack([u, uc, ux, uxc])
        ks = jnp.stack([pk, kc, kx, kxc])
        ps = ks[..., :top].astype(jnp.int32) - lax.axis_index('ep') * (el * cap)
        hit = ps[..., None] == jnp.arange(el * cap, dtype=jnp.int32)
        disp = jnp.any(hit, axis=-2).astype(jnp.bfloat16)
        comb = jnp.sum(jnp.where(hit, ks[..., top:, None], 0.0), axis=-2)
        x = _mm('gtr,gtd->grd', disp, us).astype(jnp.bfloat16).reshape(4, el, cap, d)
        y = _experts(x, ue1, ue3, ue2).reshape(4, el * cap, d)
        m = sum(_mm('gtr,grd->gtd', p, y) for p in _parts(comb))
        got = lax.ppermute(jnp.stack([m[1], m[3]]), 'ep', core)
        far = lax.ppermute(m[2] + got[1], 'ep', chip)
        out = a.astype(jnp.float32) + fo + (m[0] + got[0] + far).reshape(b, s, d)
        return out.astype(jnp.bfloat16)

    specs = (rows, rows, rows) + (rep,) * 11 + (P('ep'), P('ep'), P('ep'))
    return jax.shard_map(local, mesh=mesh, in_specs=specs, out_specs=rows, check_vma=False)
```

```python
import functools

import jax
import jax.numpy as jnp
from jax import lax
from jax.experimental import pallas as pl
from jax.experimental.pallas import tpu as pltpu
from jax.sharding import PartitionSpec as P

HEAD = 128
EPS = 1e-6
CAP_FACTOR = 2
WIDE = 512
BLK = 256
RING = 8
WSLOTS = 3
MESH = pl.DeviceIdType.MESH
F32, BF16 = jnp.float32, jnp.bfloat16


def _dot(a, b):
    return jnp.dot(a, b, preferred_element_type=F32)


def _rms(x, w):
    xf = x.astype(F32)
    r = lax.rsqrt(jnp.mean(xf * xf, axis=-1, keepdims=True) + EPS)
    return (xf * r * w.astype(F32)).astype(BF16)


def _silu_mul(h1, h3):
    return (h1 * jax.nn.sigmoid(h1) * h3).astype(BF16)


def _gate(u, wr, gi):
    lg = _dot(u, wr)
    hit = gi[..., None] == jnp.arange(wr.shape[1], dtype=gi.dtype)
    return jax.nn.softmax(jnp.sum(jnp.where(hit, lg[:, None, :], 0.0), axis=-1), axis=-1)


def _tables(s):
    half = HEAD // 2
    freq = 10000.0 ** (-jnp.arange(half, dtype=F32) / half)
    ang = jnp.arange(s, dtype=F32)[:, None] * freq[None, :]
    c, sn = jnp.cos(ang), jnp.sin(ang)
    return jnp.concatenate([c, c], axis=-1), jnp.concatenate([-sn, sn], axis=-1)


def _dense_kernel(na, nf, h_ref, la_ref, lf_ref, cos_ref, sin_ref, wq_ref, wk_ref, wv_ref, wo_ref, w1_ref, w3_ref, w2_ref,
                  out_ref, x_ref, acc_ref):
    g = pl.program_id(0)
    t = h_ref.shape[0]

    @pl.when(g == 0)
    def _():
        x_ref[...] = _rms(h_ref[...], la_ref[...])
        acc_ref[...] = jnp.zeros_like(acc_ref)

    @pl.when(g < na)
    def _():
        x = x_ref[...]
        q = _dot(x, wq_ref[...])
        k = _dot(x, wk_ref[...])
        v = _dot(x, wv_ref[...]).astype(BF16)
        c, s = cos_ref[...], sin_ref[...]
        ok = lax.broadcasted_iota(jnp.int32, (t, t), 0) >= lax.broadcasted_iota(jnp.int32, (t, t), 1)
        outs = []
        for i in range(WIDE // HEAD):
            cols = slice(i * HEAD, (i + 1) * HEAD)
            qi, ki = q[:, cols], k[:, cols]
            qi = (qi * c + pltpu.roll(qi, HEAD // 2, 1) * s).astype(BF16)
            ki = (ki * c + pltpu.roll(ki, HEAD // 2, 1) * s).astype(BF16)
            sc = lax.dot_general(qi, ki, (((1,), (1,)), ((), ())), preferred_element_type=F32) * HEAD ** -0.5
            sc = jnp.where(ok, sc, -1e30)
            e = jnp.exp(sc - jnp.max(sc, axis=-1, keepdims=True))
            p = (e / jnp.sum(e, axis=-1, keepdims=True)).astype(BF16)
            outs.append(_dot(p, v[:, cols]).astype(BF16))
        acc_ref[...] += _dot(jnp.concatenate(outs, axis=-1), wo_ref[...])

    @pl.when(g == na - 1)
    def _():
        a = (h_ref[...].astype(F32) + acc_ref[...]).astype(BF16)
        acc_ref[...] = a.astype(F32)
        x_ref[...] = _rms(a, lf_ref[...])

    @pl.when(g >= na)
    def _():
        x = x_ref[...]
        s = _silu_mul(_dot(x, w1_ref[...]), _dot(x, w3_ref[...]))
        acc_ref[...] += _dot(s, w2_ref[...])

    @pl.when(g == na + nf - 1)
    def _():
        for c in range(out_ref.shape[0]):
            out_ref[c] = acc_ref[:, c * BLK:(c + 1) * BLK]


def _dense(h, ln_attn, wq, wk, wv, wo, ln_ffn, ws1, ws3, ws2):
    t, d = h.shape
    na, nf = wq.shape[1] // WIDE, ws1.shape[1] // BLK
    cos, sin = _tables(t)
    full = lambda shape: pl.BlockSpec(shape, lambda g: (0,) * len(shape))
    head = lambda g: jnp.minimum(g, na - 1)
    ffn = lambda g: jnp.maximum(g - na, 0)
    col = lambda w, f: pl.BlockSpec((d, w), lambda g: (0, f(g)))
    row = lambda w, f: pl.BlockSpec((w, d), lambda g: (f(g), 0))
    return pl.pallas_call(
        functools.partial(_dense_kernel, na, nf),
        grid=(na + nf,),
        in_specs=[full((t, d)), full((1, d)), full((1, d)), full((t, HEAD)), full((t, HEAD)),
                  col(WIDE, head), col(WIDE, head), col(WIDE, head), row(WIDE, head),
                  col(BLK, ffn), col(BLK, ffn), row(BLK, ffn)],
        out_specs=full((d // BLK, t, BLK)),
        out_shape=jax.ShapeDtypeStruct((d // BLK, t, BLK), F32),
        scratch_shapes=[pltpu.VMEM((t, d), BF16), pltpu.VMEM((t, d), F32)],
        compiler_params=pltpu.CompilerParams(dimension_semantics=('arbitrary',), vmem_limit_bytes=56 << 20),
        cost_estimate=pl.CostEstimate(flops=2 * t * d * (4 * d + 3 * ws1.shape[1]), transcendentals=0,
                                      bytes_accessed=2 * d * (4 * d + 3 * ws1.shape[1])),
        name='dense',
    )(h, ln_attn[None], ln_ffn[None], cos, sin, wq, wk, wv, wo, ws1, ws3, ws2)


def _expert_kernel(el, cap, top, u0, u1, u2, u3, pt_ref, pk_ref, base_hbm, ue1, ue3, ue2, out_hbm,
                   wbuf, ring, he, ub, xs, ys, cm, sd, rd, sx, rx, base, ob,
                   wsem, rsem, usem, bsem, osem, sd_sem, rd_sem, sx_sem, rx_sem):
    me = lax.axis_index('ep')
    dp = lax.axis_index('dp')
    core = (dp, me + 1 - 2 * lax.rem(me, 2))
    chip = (dp, lax.rem(me + 2, 4))
    fe = ue1.shape[2]
    wa = (fe // 2 + 127) // 128 * 128
    widths = (wa, fe - wa)
    nc = out_hbm.shape[1] // BLK
    first = me * (el * cap)

    def unit(e, h, slot):
        w, lo = widths[h], h * wa
        return [pltpu.make_async_copy(ue.at[e, :, lo:lo + w], wbuf.at[slot, :, k * w:(k + 1) * w], wsem.at[slot, k])
                for k, ue in enumerate((ue1, ue3))]

    def piece(c, e, slot):
        return pltpu.make_async_copy(ue2.at[e, :, pl.ds(pl.multiple_of(c * BLK, BLK), BLK)], ring.at[slot], rsem.at[slot])

    ucopies = [pltpu.make_async_copy(r, ub.at[k], usem.at[k]) for k, r in enumerate((u0, u1, u2, u3))]
    for cp in ucopies:
        cp.start()
    for n in range(WSLOTS):
        for cp in unit(n // 2, n % 2, n):
            cp.start()
    bcopy = pltpu.make_async_copy(base_hbm, base, bsem)
    bcopy.start()

    barrier = pltpu.get_barrier_semaphore()
    for peer in (core, chip):
        pl.semaphore_signal(barrier, inc=1, device_id=peer, device_id_type=MESH)
    pl.semaphore_wait(barrier, 2)

    for k in range(4):
        pos, gate = pk_ref[k, :, :top], pk_ref[k, :, top:2 * top]
        r = (lax.broadcasted_iota(jnp.int32, (pos.shape[0], el * cap), 1) + first).astype(F32)
        c = jnp.zeros(r.shape, F32)
        for j in range(top):
            c += jnp.where(pos[:, j:j + 1] == r, gate[:, j:j + 1], 0.0)
        hi = c.astype(BF16)
        c -= hi.astype(F32)
        mid = c.astype(BF16)
        cm[0, k] = hi
        cm[1, k] = mid
        cm[2, k] = (c - mid.astype(F32)).astype(BF16)

    for cp in ucopies:
        cp.wait()

    def ffn_in(e, _):
        for k in range(4):
            r = lax.broadcasted_iota(jnp.int32, (cap, pt_ref.shape[2]), 0) + (first + e * cap)
            hit = pt_ref[k, 0:1, :] == r
            for j in range(1, top):
                hit = jnp.logical_or(hit, pt_ref[k, j:j + 1, :] == r)
            xs[k * cap:(k + 1) * cap, :] = _dot(hit.astype(F32).astype(BF16), ub[k]).astype(BF16)
        for h in range(2):
            n = 2 * e + h
            slot = lax.rem(n, WSLOTS)
            w = widths[h]
            for cp in unit(e, h, slot):
                cp.wait()
            z = _dot(xs[...], wbuf[slot, :, :2 * w])
            he[e, :, h * wa:h * wa + w] = _silu_mul(z[:, :w], z[:, w:])
            en, hn = e + (h + WSLOTS) // 2, (h + WSLOTS) % 2

            @pl.when(en < el)
            def _():
                for cp in unit(en, hn, slot):
                    cp.start()
        return 0

    lax.fori_loop(0, el - 1, ffn_in, 0)
    for n in range(RING):
        piece(0, n, n).start()
    ffn_in(el - 1, 0)
    bcopy.wait()

    def d2d(c, k):
        return pltpu.make_async_remote_copy(sd.at[lax.rem(c, 2), k], rd.at[c, k], sd_sem.at[lax.rem(c, 2), k], rd_sem.at[c, k],
                                            device_id=core, device_id_type=MESH)

    def x2x(c):
        return pltpu.make_async_remote_copy(sx.at[c], rx.at[c], sx_sem.at[c], rx_sem.at[c],
                                            device_id=chip, device_id_type=MESH)

    def relay(c):
        d2d(c, 1).wait_recv()
        sx[c] += rd[c, 1]
        x2x(c).start()
        d2d(c, 0).wait_recv()
        base[c] += rd[c, 0]

    def chunk(c, _):
        def pair(i, _):
            for h in range(2):
                e = 2 * i + h
                slot = lax.rem(e, RING)
                piece(c, e, slot).wait()
                y = _dot(he[e], ring[slot]).astype(BF16)
                for k in range(4):
                    ys[k, pl.ds(pl.multiple_of(e * cap, cap), cap), :] = y[k * cap:(k + 1) * cap]
                wrap = (e + RING >= el).astype(jnp.int32)

                @pl.when(c + wrap < nc)
                def _():
                    piece(c + wrap, lax.rem(e + RING, el), slot).start()
            return 0

        lax.fori_loop(0, el // 2, pair, 0)

        @pl.when(c >= 2)
        def _():
            for k in range(2):
                d2d(c - 2, k).wait_send()

        def total(k):
            return _dot(cm[0, k], ys[k]) + _dot(cm[1, k], ys[k]) + _dot(cm[2, k], ys[k])

        sd[lax.rem(c, 2), 1] = total(3)
        d2d(c, 1).start()
        sd[lax.rem(c, 2), 0] = total(1)
        d2d(c, 0).start()
        sx[c] = total(2)
        base[c] += total(0)

        @pl.when(c >= 1)
        def _():
            relay(c - 1)
        return 0

    lax.fori_loop(0, nc, chunk, 0)
    relay(nc - 1)
    for c in (nc - 2, nc - 1):
        for k in range(2):
            d2d(c, k).wait_send()

    def put(c):
        return pltpu.make_async_copy(ob.at[c], out_hbm.at[:, pl.ds(pl.multiple_of(c * BLK, BLK), BLK)], osem.at[c])

    def finish(c, _):
        x2x(c).wait_recv()
        ob[c] = (base[c] + rx[c]).astype(BF16)
        put(c).start()
        return 0

    lax.fori_loop(0, nc, finish, 0)

    def drain(c, _):
        x2x(c).wait_send()
        put(c).wait()
        return 0

    lax.fori_loop(0, nc, drain, 0)


def _experts(us, pt, pk, base, ue1, ue3, ue2, top, cap):
    t, d = us[0].shape
    el, _, fe = ue1.shape
    nc = d // BLK
    wa = (fe // 2 + 127) // 128 * 128
    hbm = pl.BlockSpec(memory_space=pl.ANY)
    vmem = pl.BlockSpec(memory_space=pltpu.VMEM)
    dma = pltpu.SemaphoreType.DMA
    return pl.pallas_call(
        functools.partial(_expert_kernel, el, cap, top),
        in_specs=[hbm] * 4 + [vmem] * 2 + [hbm] * 4,
        out_specs=hbm,
        out_shape=jax.ShapeDtypeStruct((t, d), BF16),
        scratch_shapes=[
            pltpu.VMEM((WSLOTS, d, 2 * wa), BF16), pltpu.VMEM((RING, fe, BLK), BF16), pltpu.VMEM((el, 4 * cap, fe), BF16),
            pltpu.VMEM((4, t, d), BF16), pltpu.VMEM((4 * cap, d), BF16), pltpu.VMEM((4, el * cap, BLK), BF16),
            pltpu.VMEM((3, 4, t, el * cap), BF16), pltpu.VMEM((2, 2, t, BLK), F32), pltpu.VMEM((nc, 2, t, BLK), F32),
            pltpu.VMEM((nc, t, BLK), F32), pltpu.VMEM((nc, t, BLK), F32), pltpu.VMEM((nc, t, BLK), F32),
            pltpu.VMEM((nc, t, BLK), BF16),
            dma((WSLOTS, 2)), dma((RING,)), dma((4,)), dma, dma((nc,)), dma((2, 2)), dma((nc, 2)), dma((nc,)), dma((nc,)),
        ],
        compiler_params=pltpu.CompilerParams(collective_id=0, has_side_effects=True, vmem_limit_bytes=67043328),
        cost_estimate=pl.CostEstimate(flops=6 * el * 4 * cap * d * fe, transcendentals=0, bytes_accessed=6 * el * d * fe),
        name='experts',
    )(*us, pt, pk, base, ue1, ue3, ue2)


def solution(mesh):
    rows = P(('dp', 'ep'))
    rep = P()
    core = [(k, k ^ 1) for k in range(4)]
    chip = [(k, k ^ 2) for k in range(4)]

    def local(h0, idx, slot, ln_attn, wq, wk, wv, wo, ln_ffn, ws1, ws3, ws2, ln_moe, wr, ue1, ue3, ue2):
        b, s, d = h0.shape
        top = idx.shape[-1]
        el = ue1.shape[0]
        t = b * s
        cap = CAP_FACTOR * t * top // (el * mesh.shape['ep'])
        h = h0.reshape(t, d)
        u = _rms(h, ln_moe)
        gi = idx.reshape(t, top)
        gate = _gate(u, wr, gi)
        pos = (gi * cap + slot.reshape(t, top)).astype(F32)
        pk = jnp.concatenate([pos, gate], axis=-1)
        ux, kx = lax.ppermute(u, 'ep', chip), lax.ppermute(pk, 'ep', chip)
        uc, kc = lax.ppermute(u, 'ep', core), lax.ppermute(pk, 'ep', core)
        uxc, kxc = lax.ppermute(ux, 'ep', core), lax.ppermute(kx, 'ep', core)
        base = _dense(h, ln_attn, wq, wk, wv, wo, ln_ffn, ws1, ws3, ws2)
        ks = jnp.stack([pk, kc, kx, kxc])
        pt = jnp.transpose(ks[..., :top], (0, 2, 1)).astype(jnp.int32)
        out = _experts((u, uc, ux, uxc), pt, ks, base, ue1, ue3, ue2, top, cap)
        return out.reshape(b, s, d)

    specs = (rows, rows, rows) + (rep,) * 11 + (P('ep'), P('ep'), P('ep'))
    return jax.shard_map(local, mesh=mesh, in_specs=specs, out_specs=rows, check_vma=False)
```

```python
import functools

import jax
import jax.numpy as jnp
import numpy as np
from jax import lax
from jax.experimental import pallas as pl
from jax.experimental.pallas import tpu as pltpu
from jax.sharding import PartitionSpec as P

HEAD = 128
EPS = 1e-6
CAP_FACTOR = 2
BLK = 256
RING = 8
SLOTS = 3
GROUP = 4
PIECES = 4
MESH = pl.DeviceIdType.MESH
F32, BF16 = jnp.float32, jnp.bfloat16


def _dot(a, b):
    return jnp.dot(a, b, preferred_element_type=F32)


def _rms(x, w):
    xf = x.astype(F32)
    r = lax.rsqrt(jnp.mean(xf * xf, axis=-1, keepdims=True) + EPS)
    return (xf * r * w).astype(BF16)


def _silu_mul(h1, h3):
    return (h1 * jax.nn.sigmoid(h1) * h3).astype(BF16)


def _tables(s):
    half = HEAD // 2
    freq = np.float32(10000.0) ** (-np.arange(half, dtype=np.float32) / np.float32(half))
    ang = np.arange(s, dtype=np.float32)[:, None] * freq[None, :]
    c, sn = np.cos(ang), np.sin(ang)
    return np.stack([np.concatenate([c, c], axis=-1), np.concatenate([-sn, sn], axis=-1)]).astype(np.float32)


def _layer(el, cap, top, h_ref, pt_ref, ln_ref, tab_ref, wr_ref, wq, wk, wv, wo, ws1, ws3, ws2, ue1, ue3, ue2, out_hbm,
           wbuf, ring, he, ub, xa, sb, x4, ys, cm, pts, sd, rd, sx, rx, base, ob,
           wsem, rsem, osem, hs_sem, hr_sem, ps_sem, pr_sem, sd_sem, rd_sem, sx_sem, rx_sem):
    me = lax.axis_index('ep')
    dp = lax.axis_index('dp')
    core = (dp, me + 1 - 2 * lax.rem(me, 2))
    chip = (dp, lax.rem(me + 2, 4))
    t, d = h_ref.shape
    fe, fs = ue1.shape[2], ws1.shape[1]
    wide = wbuf.shape[2]
    wa = wide // 2
    widths = (wa, fe - wa)
    nc = d // BLK
    hw = wide // 3
    na = d // hw
    first = me * (el * cap)

    def load(src, dst, sem):
        return pltpu.make_async_copy(src, dst, sem)

    def send(src, dst, s, r, peer):
        return pltpu.make_async_remote_copy(src, dst, s, r, device_id=peer, device_id_type=MESH)

    def qkv(i, slot):
        cols = pl.ds(pl.multiple_of(i * hw, hw), hw)
        return [load(w.at[:, cols], wbuf.at[slot, :, k * hw:(k + 1) * hw], wsem.at[slot, k])
                for k, w in enumerate((wq, wk, wv))]

    wo_a = [load(wo.at[:, :wide], wbuf.at[na % SLOTS], wsem.at[na % SLOTS, 0])]
    wo_b = [load(wo.at[:, wide:], wbuf.at[(na + 1) % SLOTS, :, :d - wide], wsem.at[(na + 1) % SLOTS, 0])]

    def unit(e, h, slot):
        w, lo = widths[h], h * wa
        return [load(ue.at[e, :, lo:lo + w], wbuf.at[slot, :, k * w:(k + 1) * w], wsem.at[slot, k])
                for k, ue in enumerate((ue1, ue3))]

    def piece(c, e, slot):
        return load(ue2.at[e, :, pl.ds(pl.multiple_of(c * BLK, BLK), BLK)], ring.at[slot], rsem.at[slot])

    def shared_in(k):
        lo, w = k * wa, min(wa, fs - k * wa)
        return [load(ws.at[:, lo:lo + w], wbuf.at[k % SLOTS, :, i * w:(i + 1) * w], wsem.at[k % SLOTS, i])
                for i, ws in enumerate((ws1, ws3))]

    ns = -(-fs // wa)
    slot_a, slot_b = ns % SLOTS, (ns + 1) % SLOTS
    rest, tail = fs - d, d - wide
    half = wide - tail
    shared_a = [load(ws2.at[:d, :wide], wbuf.at[slot_a], wsem.at[slot_a, 0])]
    shared_b = [load(ws2.at[:d, wide:], wbuf.at[slot_b, :, :tail], wsem.at[slot_b, 0]),
                load(ws2.at[d:, :half], wbuf.at[slot_b, :rest, tail:], wsem.at[slot_b, 1]),
                load(ws2.at[d:, half:], wbuf.at[slot_b, rest:2 * rest, tail:], wsem.at[slot_b, 2])]

    def start(copies):
        for cp in copies:
            cp.start()

    def wait(copies):
        for cp in copies:
            cp.wait()

    for n in range(SLOTS):
        start(qkv(n, n))

    barrier = pltpu.get_barrier_semaphore()
    for peer in (core, chip):
        pl.semaphore_signal(barrier, inc=1, device_id=peer, device_id_type=MESH)
    pl.semaphore_wait(barrier, 2)

    rows = t // PIECES
    part = [pl.ds(q * rows, rows) for q in range(PIECES)]
    far = [send(h_ref.at[part[q]], ub.at[2, part[q]], hs_sem.at[q], hr_sem.at[q], chip) for q in range(PIECES)]
    near = send(h_ref, ub.at[1], hs_sem.at[PIECES], hr_sem.at[PIECES], core)
    onward = [send(ub.at[2, part[q]], ub.at[3, part[q]], hs_sem.at[PIECES + 1 + q], hr_sem.at[PIECES + 1 + q], core)
              for q in range(PIECES)]
    pfar = send(pt_ref, pts.at[2], ps_sem.at[0], pr_sem.at[0], chip)
    pnear = send(pt_ref, pts.at[1], ps_sem.at[1], pr_sem.at[1], core)
    ponward = send(pts.at[2], pts.at[3], ps_sem.at[2], pr_sem.at[2], core)
    pfar.start()
    start(far)
    pnear.start()
    near.start()

    xa[...] = _rms(h_ref[...], ln_ref[0:1, :])
    ub[0] = _rms(h_ref[...], ln_ref[2:3, :])
    pts[0] = pt_ref[...]

    def heads(i, _):
        slot = lax.rem(i, SLOTS)
        wait(qkv(i, slot))
        z = _dot(xa[...], wbuf[slot])

        @pl.when(i + SLOTS < na)
        def _():
            start(qkv(i + SLOTS, slot))

        for k, nxt in enumerate((wo_a, wo_b, unit(0, 0, (na + 2) % SLOTS))):
            @pl.when(i + SLOTS == na + k)
            def _():
                start(nxt)

        c, s = tab_ref[0], tab_ref[1]
        ok = lax.broadcasted_iota(jnp.int32, (t, t), 0) >= lax.broadcasted_iota(jnp.int32, (t, t), 1)
        outs = []
        for j in range(hw // HEAD):
            qj, kj, vj = (z[:, m * hw + j * HEAD:m * hw + (j + 1) * HEAD] for m in range(3))
            qj = (qj * c + pltpu.roll(qj, HEAD // 2, 1) * s).astype(BF16)
            kj = (kj * c + pltpu.roll(kj, HEAD // 2, 1) * s).astype(BF16)
            sc = lax.dot_general(qj, kj, (((1,), (1,)), ((), ())), preferred_element_type=F32) * HEAD ** -0.5
            sc = jnp.where(ok, sc, -1e30)
            e = jnp.exp(sc - jnp.max(sc, axis=-1, keepdims=True))
            p = (e / jnp.sum(e, axis=-1, keepdims=True)).astype(BF16)
            outs.append(_dot(p, vj.astype(BF16)).astype(BF16))
        sb[:, pl.ds(pl.multiple_of(i * hw, hw), hw)] = jnp.concatenate(outs, axis=-1)
        return 0

    lax.fori_loop(0, na, heads, 0)

    def pass_on(q):
        far[q].wait_recv()
        onward[q].start()

    pfar.wait_recv()
    ponward.start()
    pass_on(0)
    pass_on(1)

    def residual(z, lo):
        a = (h_ref[:, lo:lo + z.shape[1]].astype(F32) + z).astype(BF16)
        xa[:, lo:lo + z.shape[1]] = a
        for c in range(z.shape[1] // BLK):
            base[lo // BLK + c] = a[:, c * BLK:(c + 1) * BLK].astype(F32)

    wait(wo_a)
    residual(_dot(sb[:, :d], wbuf[na % SLOTS]), 0)
    start(unit(0, 1, na % SLOTS))
    wait(wo_b)
    residual(_dot(sb[:, :d], wbuf[(na + 1) % SLOTS, :, :d - wide]), wide)
    start(unit(1, 0, (na + 1) % SLOTS))
    xa[...] = _rms(xa[...], ln_ref[1:2, :])
    pass_on(2)

    def weigh(k):
        pos = jnp.concatenate([pts[k].astype(F32), jnp.zeros((HEAD - pts.shape[1], t), F32)], axis=0).T
        lg = _dot(ub[k], wr_ref[...])
        lo = lax.broadcasted_iota(jnp.int32, lg.shape, 1).astype(F32) * cap
        picks = []
        for j in range(top):
            off = pos[:, j:j + 1] - lo
            hit = jnp.logical_and(off >= 0, off < cap)
            picks.append(jnp.sum(jnp.where(hit, lg, 0.0), axis=-1, keepdims=True))
        big = functools.reduce(jnp.maximum, picks)
        ex = [jnp.exp(p - big) for p in picks]
        tot = functools.reduce(jnp.add, ex)
        r = (lax.broadcasted_iota(jnp.int32, (t, el * cap), 1) + first).astype(F32)
        c = jnp.zeros(r.shape, F32)
        for j in range(top):
            c += jnp.where(pos[:, j:j + 1] == r, ex[j] / tot, 0.0)
        hi = c.astype(BF16)
        c -= hi.astype(F32)
        mid = c.astype(BF16)
        cm[k, :t] = hi
        cm[k, t:2 * t] = mid
        cm[k, 2 * t:] = (c - mid.astype(F32)).astype(BF16)

    near.wait_recv()
    pnear.wait_recv()
    ub[1] = _rms(ub[1], ln_ref[2:3, :])

    def weigh_body(k, _):
        weigh(k)
        return 0

    lax.fori_loop(0, 2, weigh_body, 0)
    pass_on(3)
    for cp in onward:
        cp.wait_send()
    ub[2] = _rms(ub[2], ln_ref[2:3, :])
    for cp in onward:
        cp.wait_recv()
    ub[3] = _rms(ub[3], ln_ref[2:3, :])
    ponward.wait()
    pfar.wait_send()
    pnear.wait_send()
    near.wait_send()
    for cp in far:
        cp.wait_send()

    off = (na + 2) % SLOTS

    def group(g, last):
        for k in range(4):
            r = lax.broadcasted_iota(jnp.int32, (GROUP * cap, t), 0) + (first + g * (GROUP * cap))
            hit = pts[k, 0:1, :] == r
            for j in range(1, top):
                hit = jnp.logical_or(hit, pts[k, j:j + 1, :] == r)
            x = _dot(hit.astype(F32).astype(BF16), ub[k]).astype(BF16)
            for j in range(GROUP):
                x4[j, k * cap:(k + 1) * cap, :] = x[j * cap:(j + 1) * cap]

        @pl.when(g < 2)
        def _():
            weigh(g + 2)

        def ffn_in(j, _):
            e = g * GROUP + j
            for h in range(2):
                slot = lax.rem(2 * e + h + off, SLOTS)
                w = widths[h]
                wait(unit(e, h, slot))
                z = _dot(x4[j], wbuf[slot, :, :2 * w])
                he[e, :, h * wa:h * wa + w] = _silu_mul(z[:, :w], z[:, w:])
                en, hn = e + (h + SLOTS) // 2, (h + SLOTS) % 2

                @pl.when(en < el)
                def _():
                    start(unit(en, hn, slot))

                if h == 0:
                    @pl.when(e == el - 1)
                    def _():
                        for n in range(RING):
                            piece(0, n, n).start()
            return 0

        lax.fori_loop(0, GROUP, ffn_in, 0)
        return last

    lax.fori_loop(0, el // GROUP, group, 0)

    def d2d(c, k):
        p = lax.rem(c, 2)
        return send(sd.at[p, k], rd.at[p, k], sd_sem.at[p, k], rd_sem.at[p, k], core)

    def x2x(c):
        return send(sx.at[c], rx.at[c], sx_sem.at[c], rx_sem.at[c], chip)

    def chunk(c, _):
        def quad(i, _):
            s0 = GROUP * lax.rem(i, RING // GROUP)
            for k in range(GROUP):
                piece(c, GROUP * i + k, s0 + k).wait()
            for k in range(GROUP):
                e = GROUP * i + k
                y = _dot(he[e], ring[s0 + k]).astype(BF16)
                for b in range(4):
                    ys[b, pl.ds(pl.multiple_of(e * cap, cap), cap), :] = y[b * cap:(b + 1) * cap]
            wrap = (GROUP * i + RING >= el).astype(jnp.int32)

            @pl.when(c + wrap < nc)
            def _():
                for k in range(GROUP):
                    piece(c + wrap, lax.rem(GROUP * i + RING, el) + k, s0 + k).start()
            return 0

        lax.fori_loop(0, el // GROUP, quad, 0)

        for k in range(SLOTS):
            @pl.when(c == k + 1)
            def _():
                start(shared_in(k))

        @pl.when(c >= 2)
        def _():
            for k in range(2):
                d2d(c - 2, k).wait_send()

        def total(k):
            z = _dot(cm[k], ys[k])
            return z[:t] + z[t:2 * t] + z[2 * t:]

        sd[lax.rem(c, 2), 1] = total(3)
        d2d(c, 1).start()
        sx[c] = total(2)
        sd[lax.rem(c, 2), 0] = total(1)
        d2d(c, 0).start()
        base[c] += total(0)
        d2d(c, 1).wait_recv()
        sx[c] += rd[lax.rem(c, 2), 1]
        x2x(c).start()
        d2d(c, 0).wait_recv()
        base[c] += rd[lax.rem(c, 2), 0]
        return 0

    lax.fori_loop(0, nc, chunk, 0)
    for c in (nc - 2, nc - 1):
        for k in range(2):
            d2d(c, k).wait_send()

    for k in range(ns):
        wait(shared_in(k))
        w = min(wa, fs - k * wa)
        z = _dot(xa[...], wbuf[k % SLOTS, :, :2 * w])
        sb[:, k * wa:k * wa + w] = _silu_mul(z[:, :w], z[:, w:])
        if k + SLOTS < ns:
            start(shared_in(k + SLOTS))
        elif k + SLOTS == ns:
            start(shared_a)
        elif k + SLOTS == ns + 1:
            start(shared_b)

    def add(z, lo):
        for c in range(z.shape[1] // BLK):
            base[lo // BLK + c] += z[:, c * BLK:(c + 1) * BLK]

    wait(shared_a)
    add(_dot(sb[:, :d], wbuf[slot_a]), 0)
    wait(shared_b)
    add(_dot(sb[:, :d], wbuf[slot_b, :, :tail]), wide)
    add(_dot(sb[:, d:], wbuf[slot_b, :rest, tail:]), 0)
    add(_dot(sb[:, d:], wbuf[slot_b, rest:2 * rest, tail:]), half)

    def put(c):
        return load(ob.at[c], out_hbm.at[:, pl.ds(pl.multiple_of(c * BLK, BLK), BLK)], osem.at[c])

    def finish(c, _):
        x2x(c).wait_recv()
        ob[c] = (base[c] + rx[c]).astype(BF16)
        put(c).start()
        return 0

    lax.fori_loop(0, nc, finish, 0)

    def drain(c, _):
        x2x(c).wait_send()
        put(c).wait()
        return 0

    lax.fori_loop(0, nc, drain, 0)


def solution(mesh):
    rows = P(('dp', 'ep'))
    rep = P()

    def local(h0, idx, slot, ln_attn, wq, wk, wv, wo, ln_ffn, ws1, ws3, ws2, ln_moe, wr, ue1, ue3, ue2):
        b, s, d = h0.shape
        top = idx.shape[-1]
        el, _, fe = ue1.shape
        fs = ws1.shape[1]
        t = b * s
        cap = CAP_FACTOR * t * top // (el * mesh.shape['ep'])
        nc = d // BLK
        wide = 2 * ((fe // 2 + HEAD - 1) // HEAD * HEAD)
        pos = (idx * cap + slot).reshape(t, top)
        pt = jnp.pad(pos.T, ((0, 8 - top), (0, 0)), constant_values=-1)
        lns = jnp.stack([ln_attn, ln_ffn, ln_moe]).astype(F32)
        hbm = pl.BlockSpec(memory_space=pl.ANY)
        vmem = pl.BlockSpec(memory_space=pltpu.VMEM)
        dma = pltpu.SemaphoreType.DMA
        out = pl.pallas_call(
            functools.partial(_layer, el, cap, top),
            in_specs=[vmem] * 5 + [hbm] * 10,
            out_specs=hbm,
            out_shape=jax.ShapeDtypeStruct((t, d), BF16),
            scratch_shapes=[
                pltpu.VMEM((SLOTS, d, wide), BF16), pltpu.VMEM((RING, fe, BLK), BF16), pltpu.VMEM((el, 4 * cap, fe), BF16),
                pltpu.VMEM((4, t, d), BF16), pltpu.VMEM((t, d), BF16), pltpu.VMEM((t, fs), BF16),
                pltpu.VMEM((GROUP, 4 * cap, d), BF16), pltpu.VMEM((4, el * cap, BLK), BF16),
                pltpu.VMEM((4, 3 * t, el * cap), BF16), pltpu.VMEM((4, 8, t), jnp.int32),
                pltpu.VMEM((2, 2, t, BLK), F32), pltpu.VMEM((2, 2, t, BLK), F32),
                pltpu.VMEM((nc, t, BLK), F32), pltpu.VMEM((nc, t, BLK), F32), pltpu.VMEM((nc, t, BLK), F32),
                pltpu.VMEM((nc, t, BLK), BF16),
                dma((SLOTS, 3)), dma((RING,)), dma((nc,)), dma((2 * PIECES + 1,)), dma((2 * PIECES + 1,)), dma((3,)), dma((3,)),
                dma((2, 2)), dma((2, 2)), dma((nc,)), dma((nc,)),
            ],
            compiler_params=pltpu.CompilerParams(collective_id=0, has_side_effects=True, vmem_limit_bytes=67043328),
            name='layer',
        )(h0.reshape(t, d), pt, lns, jnp.asarray(_tables(s)), wr, wq, wk, wv, wo, ws1, ws3, ws2, ue1, ue3, ue2)
        return out.reshape(b, s, d)

    specs = (rows, rows, rows) + (rep,) * 11 + (P('ep'), P('ep'), P('ep'))
    return jax.shard_map(local, mesh=mesh, in_specs=specs, out_specs=rows, check_vma=False)
```

```python
import functools

import jax
import jax.numpy as jnp
import numpy as np
from jax import lax
from jax.experimental import pallas as pl
from jax.experimental.pallas import tpu as pltpu
from jax.sharding import PartitionSpec as P

HEAD = 128
EPS = 1e-6
CAP_FACTOR = 2
BLK = 256
RING = 8
SLOTS = 3
GROUP = 4
PIECES = 4
MESH = pl.DeviceIdType.MESH
F32, BF16 = jnp.float32, jnp.bfloat16


def _dot(a, b):
    return jnp.dot(a, b, preferred_element_type=F32)


def _rms(x, w):
    xf = x.astype(F32)
    r = lax.rsqrt(jnp.mean(xf * xf, axis=-1, keepdims=True) + EPS)
    return (xf * r * w).astype(BF16)


def _silu_mul(h1, h3):
    return (h1 * jax.nn.sigmoid(h1) * h3).astype(BF16)


def _tables(s):
    half = HEAD // 2
    freq = np.float32(10000.0) ** (-np.arange(half, dtype=np.float32) / np.float32(half))
    ang = np.arange(s, dtype=np.float32)[:, None] * freq[None, :]
    c, sn = np.cos(ang), np.sin(ang)
    return np.stack([np.concatenate([c, c], axis=-1), np.concatenate([-sn, sn], axis=-1)]).astype(np.float32)


def _layer(el, cap, top, idx_ref, slot_ref, la_ref, lf_ref, lm_ref, h_hbm, tab_hbm, wr_hbm, wq, wk, wv, wo, ws1, ws3, ws2, ue1, ue3, ue2, out_hbm,
           h_ref, tab_ref, wr_ref, wbuf, ring, he, ub, xa, sb, x4, ys, cm, pts, sd, rd, sx, rx, base, ob,
           isem, wsem, rsem, osem, hs_sem, hr_sem, ps_sem, pr_sem, sd_sem, rd_sem, sx_sem, rx_sem):
    me = lax.axis_index('ep')
    dp = lax.axis_index('dp')
    core = (dp, me + 1 - 2 * lax.rem(me, 2))
    chip = (dp, lax.rem(me + 2, 4))
    t, d = h_ref.shape
    fe, fs = ue1.shape[2], ws1.shape[1]
    wide = wbuf.shape[2]
    wa = wide // 2
    widths = (wa, fe - wa)
    nc = d // BLK
    hw = wide // 3
    na = d // hw
    first = me * (el * cap)

    def load(src, dst, sem):
        return pltpu.make_async_copy(src, dst, sem)

    def send(src, dst, s, r, peer):
        return pltpu.make_async_remote_copy(src, dst, s, r, device_id=peer, device_id_type=MESH)

    def qkv(i, slot):
        cols = pl.ds(pl.multiple_of(i * hw, hw), hw)
        return [load(w.at[:, cols], wbuf.at[slot, :, k * hw:(k + 1) * hw], wsem.at[slot, k])
                for k, w in enumerate((wq, wk, wv))]

    wo_a = [load(wo.at[:, :wide], wbuf.at[na % SLOTS], wsem.at[na % SLOTS, 0])]
    wo_b = [load(wo.at[:, wide:], wbuf.at[(na + 1) % SLOTS, :, :d - wide], wsem.at[(na + 1) % SLOTS, 0])]

    def unit(e, h, slot):
        w, lo = widths[h], h * wa
        return [load(ue.at[e, :, lo:lo + w], wbuf.at[slot, :, k * w:(k + 1) * w], wsem.at[slot, k])
                for k, ue in enumerate((ue1, ue3))]

    def piece(c, e, slot):
        return load(ue2.at[e, :, pl.ds(pl.multiple_of(c * BLK, BLK), BLK)], ring.at[slot], rsem.at[slot])

    def shared_in(k):
        lo, w = k * wa, min(wa, fs - k * wa)
        n = (n0 + k) % SLOTS
        return [load(ws.at[:, lo:lo + w], wbuf.at[n, :, i * w:(i + 1) * w], wsem.at[n, i])
                for i, ws in enumerate((ws1, ws3))]

    ns = -(-fs // wa)
    n0 = na + 2
    slot_a, slot_b = (n0 + ns) % SLOTS, (n0 + ns + 1) % SLOTS
    rest, tail = fs - d, d - wide
    half = wide - tail
    shared_a = [load(ws2.at[:d, :wide], wbuf.at[slot_a], wsem.at[slot_a, 0])]
    shared_b = [load(ws2.at[:d, wide:], wbuf.at[slot_b, :, :tail], wsem.at[slot_b, 0]),
                load(ws2.at[d:, :half], wbuf.at[slot_b, :rest, tail:], wsem.at[slot_b, 1]),
                load(ws2.at[d:, half:], wbuf.at[slot_b, rest:2 * rest, tail:], wsem.at[slot_b, 2])]

    def start(copies):
        for cp in copies:
            cp.start()

    def wait(copies):
        for cp in copies:
            cp.wait()

    own = [load(h_hbm, h_ref, isem.at[0]), load(tab_hbm, tab_ref, isem.at[1]), load(wr_hbm, wr_ref, isem.at[2])]
    start(own)
    for n in range(SLOTS):
        start(qkv(n, n))
    pts[0] = jnp.concatenate([idx_ref[j] * cap + slot_ref[j] for j in range(top)]
                             + [jnp.full((pts.shape[1] - top, t), -1, jnp.int32)], axis=0)
    ln_a, ln_f, ln_m = (r[...].astype(F32).reshape(1, d) for r in (la_ref, lf_ref, lm_ref))

    barrier = pltpu.get_barrier_semaphore()
    for peer in (core, chip):
        pl.semaphore_signal(barrier, inc=1, device_id=peer, device_id_type=MESH)
    pl.semaphore_wait(barrier, 2)

    rows = t // PIECES
    part = [pl.ds(q * rows, rows) for q in range(PIECES)]
    far = [send(h_hbm.at[part[q]], ub.at[2, part[q]], hs_sem.at[q], hr_sem.at[q], chip) for q in range(PIECES)]
    near = send(h_hbm, ub.at[1], hs_sem.at[PIECES], hr_sem.at[PIECES], core)
    onward = [send(ub.at[2, part[q]], ub.at[3, part[q]], hs_sem.at[PIECES + 1 + q], hr_sem.at[PIECES + 1 + q], core)
              for q in range(PIECES)]
    pfar = send(pts.at[0], pts.at[2], ps_sem.at[0], pr_sem.at[0], chip)
    pnear = send(pts.at[0], pts.at[1], ps_sem.at[1], pr_sem.at[1], core)
    ponward = send(pts.at[2], pts.at[3], ps_sem.at[2], pr_sem.at[2], core)
    start(far)
    near.start()
    wait(own)

    xa[...] = _rms(h_ref[...], ln_a)
    ub[0] = _rms(h_ref[...], ln_m)
    pfar.start()
    pnear.start()

    def heads(i, _):
        slot = lax.rem(i, SLOTS)
        wait(qkv(i, slot))
        z = _dot(xa[...], wbuf[slot])

        @pl.when(i + SLOTS < na)
        def _():
            start(qkv(i + SLOTS, slot))

        for k, nxt in enumerate((wo_a, wo_b, shared_in(0))):
            @pl.when(i + SLOTS == na + k)
            def _():
                start(nxt)

        c, s = tab_ref[0], tab_ref[1]
        ok = lax.broadcasted_iota(jnp.int32, (t, t), 0) >= lax.broadcasted_iota(jnp.int32, (t, t), 1)
        outs = []
        for j in range(hw // HEAD):
            qj, kj, vj = (z[:, m * hw + j * HEAD:m * hw + (j + 1) * HEAD] for m in range(3))
            qj = (qj * c + pltpu.roll(qj, HEAD // 2, 1) * s).astype(BF16)
            kj = (kj * c + pltpu.roll(kj, HEAD // 2, 1) * s).astype(BF16)
            sc = lax.dot_general(qj, kj, (((1,), (1,)), ((), ())), preferred_element_type=F32) * HEAD ** -0.5
            sc = jnp.where(ok, sc, -1e30)
            e = jnp.exp(sc - jnp.max(sc, axis=-1, keepdims=True))
            p = (e / jnp.sum(e, axis=-1, keepdims=True)).astype(BF16)
            outs.append(_dot(p, vj.astype(BF16)).astype(BF16))
        sb[:, pl.ds(pl.multiple_of(i * hw, hw), hw)] = jnp.concatenate(outs, axis=-1)
        return 0

    lax.fori_loop(0, na, heads, 0)

    def pass_on(q):
        far[q].wait_recv()
        onward[q].start()

    pfar.wait_recv()
    ponward.start()
    pass_on(0)
    pass_on(1)

    def residual(z, lo):
        a = (h_ref[:, lo:lo + z.shape[1]].astype(F32) + z).astype(BF16)
        xa[:, lo:lo + z.shape[1]] = a
        for c in range(z.shape[1] // BLK):
            base[lo // BLK + c] = a[:, c * BLK:(c + 1) * BLK].astype(F32)

    wait(wo_a)
    residual(_dot(sb[:, :d], wbuf[na % SLOTS]), 0)
    start(shared_in(1))
    wait(wo_b)
    residual(_dot(sb[:, :d], wbuf[(na + 1) % SLOTS, :, :d - wide]), wide)
    start(shared_in(2))
    xa[...] = _rms(xa[...], ln_f)
    off = (n0 + ns + 2) % SLOTS

    for k in range(ns):
        wait(shared_in(k))
        w = min(wa, fs - k * wa)
        z = _dot(xa[...], wbuf[(n0 + k) % SLOTS, :, :2 * w])
        sb[:, k * wa:k * wa + w] = _silu_mul(z[:, :w], z[:, w:])
        if k + SLOTS < ns:
            start(shared_in(k + SLOTS))
        elif k + SLOTS == ns:
            start(shared_a)
        elif k + SLOTS == ns + 1:
            start(shared_b)
        else:
            start(unit(0, 0, off))
        if k == 0:
            pass_on(2)

    def add(z, lo):
        for c in range(z.shape[1] // BLK):
            base[lo // BLK + c] += z[:, c * BLK:(c + 1) * BLK]

    wait(shared_a)
    add(_dot(sb[:, :d], wbuf[slot_a]), 0)
    start(unit(0, 1, slot_a))
    wait(shared_b)
    add(_dot(sb[:, :d], wbuf[slot_b, :, :tail]), wide)
    add(_dot(sb[:, d:], wbuf[slot_b, :rest, tail:]), 0)
    add(_dot(sb[:, d:], wbuf[slot_b, rest:2 * rest, tail:]), half)
    start(unit(1, 0, slot_b))

    def weigh(k):
        pos = jnp.concatenate([pts[k].astype(F32), jnp.zeros((HEAD - pts.shape[1], t), F32)], axis=0).T
        lg = lax.dot_general(ub[k], wr_ref[...], (((1,), (1,)), ((), ())), preferred_element_type=F32)
        lo = lax.broadcasted_iota(jnp.int32, lg.shape, 1).astype(F32) * cap
        picks = []
        for j in range(top):
            off = pos[:, j:j + 1] - lo
            hit = jnp.logical_and(off >= 0, off < cap)
            picks.append(jnp.sum(jnp.where(hit, lg, 0.0), axis=-1, keepdims=True))
        big = functools.reduce(jnp.maximum, picks)
        ex = [jnp.exp(p - big) for p in picks]
        tot = functools.reduce(jnp.add, ex)
        r = (lax.broadcasted_iota(jnp.int32, (t, el * cap), 1) + first).astype(F32)
        c = jnp.zeros(r.shape, F32)
        for j in range(top):
            c += jnp.where(pos[:, j:j + 1] == r, ex[j] / tot, 0.0)
        hi = c.astype(BF16)
        c -= hi.astype(F32)
        mid = c.astype(BF16)
        cm[k, :t] = hi
        cm[k, t:2 * t] = mid
        cm[k, 2 * t:] = (c - mid.astype(F32)).astype(BF16)

    near.wait_recv()
    pnear.wait_recv()
    ub[1] = _rms(ub[1], ln_m)

    def weigh_body(k, _):
        weigh(k)
        return 0

    lax.fori_loop(0, 2, weigh_body, 0)
    pass_on(3)
    for cp in onward:
        cp.wait_send()
    ub[2] = _rms(ub[2], ln_m)
    for cp in onward:
        cp.wait_recv()
    ub[3] = _rms(ub[3], ln_m)
    ponward.wait()
    pfar.wait_send()
    pnear.wait_send()
    near.wait_send()
    for cp in far:
        cp.wait_send()

    def group(g, last):
        for k in range(4):
            r = lax.broadcasted_iota(jnp.int32, (GROUP * cap, t), 0) + (first + g * (GROUP * cap))
            hit = pts[k, 0:1, :] == r
            for j in range(1, top):
                hit = jnp.logical_or(hit, pts[k, j:j + 1, :] == r)
            x = _dot(hit.astype(F32).astype(BF16), ub[k]).astype(BF16)
            for j in range(GROUP):
                x4[j, k * cap:(k + 1) * cap, :] = x[j * cap:(j + 1) * cap]

        @pl.when(g < 2)
        def _():
            weigh(g + 2)

        def ffn_in(j, _):
            e = g * GROUP + j
            for h in range(2):
                slot = lax.rem(2 * e + h + off, SLOTS)
                w = widths[h]
                wait(unit(e, h, slot))
                z = _dot(x4[j], wbuf[slot, :, :2 * w])
                he[e, :, h * wa:h * wa + w] = _silu_mul(z[:, :w], z[:, w:])
                en, hn = e + (h + SLOTS) // 2, (h + SLOTS) % 2

                @pl.when(en < el)
                def _():
                    start(unit(en, hn, slot))

                if h == 0:
                    @pl.when(e == el - 1)
                    def _():
                        for n in range(RING):
                            piece(0, n, n).start()
            return 0

        lax.fori_loop(0, GROUP, ffn_in, 0)
        return last

    lax.fori_loop(0, el // GROUP, group, 0)

    def d2d(c, k):
        p = lax.rem(c, 2)
        return send(sd.at[p, k], rd.at[p, k], sd_sem.at[p, k], rd_sem.at[p, k], core)

    def x2x(c):
        return send(sx.at[c], rx.at[c], sx_sem.at[c], rx_sem.at[c], chip)

    def settle(c):
        d2d(c, 0).wait_recv()
        base[c] += rd[lax.rem(c, 2), 0]

    def chunk(c, _):
        def quad(i, _):
            s0 = GROUP * lax.rem(i, RING // GROUP)
            for k in range(GROUP):
                piece(c, GROUP * i + k, s0 + k).wait()
            for k in range(GROUP):
                e = GROUP * i + k
                y = _dot(he[e], ring[s0 + k]).astype(BF16)
                for b in range(4):
                    ys[b, pl.ds(pl.multiple_of(e * cap, cap), cap), :] = y[b * cap:(b + 1) * cap]
            wrap = (GROUP * i + RING >= el).astype(jnp.int32)

            @pl.when(c + wrap < nc)
            def _():
                for k in range(GROUP):
                    piece(c + wrap, lax.rem(GROUP * i + RING, el) + k, s0 + k).start()
            return 0

        lax.fori_loop(0, el // GROUP, quad, 0)

        @pl.when(c >= 2)
        def _():
            for k in range(2):
                d2d(c - 2, k).wait_send()

        @pl.when(c >= 1)
        def _():
            settle(c - 1)

        def total(k):
            z = _dot(cm[k], ys[k])
            return z[:t] + z[t:2 * t] + z[2 * t:]

        sd[lax.rem(c, 2), 1] = total(3)
        d2d(c, 1).start()
        sx[c] = total(2)
        sd[lax.rem(c, 2), 0] = total(1)
        d2d(c, 0).start()
        base[c] += total(0)
        d2d(c, 1).wait_recv()
        sx[c] += rd[lax.rem(c, 2), 1]
        x2x(c).start()
        return 0

    lax.fori_loop(0, nc, chunk, 0)
    settle(nc - 1)
    for c in (nc - 2, nc - 1):
        for k in range(2):
            d2d(c, k).wait_send()

    def put(c):
        return load(ob.at[c], out_hbm.at[:, pl.ds(pl.multiple_of(c * BLK, BLK), BLK)], osem.at[c])

    def finish(c, _):
        x2x(c).wait_recv()
        ob[c] = (base[c] + rx[c]).astype(BF16)
        put(c).start()
        return 0

    lax.fori_loop(0, nc, finish, 0)

    def drain(c, _):
        x2x(c).wait_send()
        put(c).wait()
        return 0

    lax.fori_loop(0, nc, drain, 0)


def solution(mesh):
    rows = P(('dp', 'ep'))
    rep = P()

    def local(h0, idx, slot, ln_attn, wq, wk, wv, wo, ln_ffn, ws1, ws3, ws2, ln_moe, wr, ue1, ue3, ue2):
        b, s, d = h0.shape
        top = idx.shape[-1]
        el, _, fe = ue1.shape
        fs = ws1.shape[1]
        t = b * s
        cap = CAP_FACTOR * t * top // (el * mesh.shape['ep'])
        nc = d // BLK
        wide = 2 * ((fe // 2 + HEAD - 1) // HEAD * HEAD)
        hbm = pl.BlockSpec(memory_space=pl.ANY)
        vmem = pl.BlockSpec(memory_space=pltpu.VMEM)
        dma = pltpu.SemaphoreType.DMA
        out = pl.pallas_call(
            functools.partial(_layer, el, cap, top),
            in_specs=[vmem] * 5 + [hbm] * 13,
            out_specs=hbm,
            out_shape=jax.ShapeDtypeStruct((t, d), BF16),
            scratch_shapes=[
                pltpu.VMEM((t, d), BF16), pltpu.VMEM((2, s, HEAD), F32), pltpu.VMEM((wr.shape[1], d), BF16),
                pltpu.VMEM((SLOTS, d, wide), BF16), pltpu.VMEM((RING, fe, BLK), BF16), pltpu.VMEM((el, 4 * cap, fe), BF16),
                pltpu.VMEM((4, t, d), BF16), pltpu.VMEM((t, d), BF16), pltpu.VMEM((t, fs), BF16),
                pltpu.VMEM((GROUP, 4 * cap, d), BF16), pltpu.VMEM((4, el * cap, BLK), BF16),
                pltpu.VMEM((4, 3 * t, el * cap), BF16), pltpu.VMEM((4, 8, t), jnp.int32),
                pltpu.VMEM((2, 2, t, BLK), F32), pltpu.VMEM((2, 2, t, BLK), F32),
                pltpu.VMEM((nc, t, BLK), F32), pltpu.VMEM((nc, t, BLK), F32), pltpu.VMEM((nc, t, BLK), F32),
                pltpu.VMEM((nc, t, BLK), BF16),
                dma((3,)), dma((SLOTS, 3)), dma((RING,)), dma((nc,)), dma((2 * PIECES + 1,)), dma((2 * PIECES + 1,)), dma((3,)), dma((3,)),
                dma((2, 2)), dma((2, 2)), dma((nc,)), dma((nc,)),
            ],
            compiler_params=pltpu.CompilerParams(collective_id=0, has_side_effects=True, vmem_limit_bytes=67043328),
            name='layer',
        )(idx.reshape(t, 1, top).transpose(2, 1, 0), slot.reshape(t, 1, top).transpose(2, 1, 0), ln_attn, ln_ffn, ln_moe,
          h0.reshape(t, d), jnp.asarray(_tables(s)), wr.T, wq, wk, wv, wo, ws1, ws3, ws2, ue1, ue3, ue2)
        return out.reshape(b, s, d)

    specs = (rows, rows, rows) + (rep,) * 11 + (P('ep'), P('ep'), P('ep'))
    return jax.shard_map(local, mesh=mesh, in_specs=specs, out_specs=rows, check_vma=False)
```

```python
import functools

import jax
import jax.numpy as jnp
import numpy as np
from jax import lax
from jax.experimental import pallas as pl
from jax.experimental.pallas import tpu as pltpu
from jax.sharding import PartitionSpec as P

HEAD = 128
EPS = 1e-6
CAP_FACTOR = 2
BLK = 256
RING = 8
SLOTS = 3
GROUP = 4
PIECES = 4
MESH = pl.DeviceIdType.MESH
F32, BF16 = jnp.float32, jnp.bfloat16


def _dot(a, b):
    return jnp.dot(a, b, preferred_element_type=F32)


def _rms(x, w):
    xf = x.astype(F32)
    r = lax.rsqrt(jnp.mean(xf * xf, axis=-1, keepdims=True) + EPS)
    return (xf * r * w).astype(BF16)


def _silu_mul(h1, h3):
    return (h1 * jax.nn.sigmoid(h1) * h3).astype(BF16)


def _tables(s):
    half = HEAD // 2
    freq = np.float32(10000.0) ** (-np.arange(half, dtype=np.float32) / np.float32(half))
    ang = np.arange(s, dtype=np.float32)[:, None] * freq[None, :]
    c, sn = np.cos(ang), np.sin(ang)
    return np.stack([np.concatenate([c, c], axis=-1), np.concatenate([-sn, sn], axis=-1)]).astype(np.float32)


def _layer(el, cap, top, idx_ref, slot_ref, la_ref, lf_ref, lm_ref, h_hbm, tab_hbm, wr_hbm, wq, wk, wv, wo, ws1, ws3, ws2, ue1, ue3, ue2, out_hbm,
           h_ref, tab_ref, wr_ref, wbuf, ring, he, ub, xa, sb, x4, ys, cm, pts, sd, rd, sx, rx, base, ob,
           isem, wsem, rsem, osem, hs_sem, hr_sem, ps_sem, pr_sem, sd_sem, rd_sem, sx_sem, rx_sem):
    me = lax.axis_index('ep')
    dp = lax.axis_index('dp')
    core = (dp, me + 1 - 2 * lax.rem(me, 2))
    chip = (dp, lax.rem(me + 2, 4))
    t, d = h_ref.shape
    fe, fs = ue1.shape[2], ws1.shape[1]
    wide = wbuf.shape[2]
    wa = wide // 2
    widths = (wa, fe - wa)
    nc = d // BLK
    hw = wide // 3
    na = d // hw
    first = me * (el * cap)

    def load(src, dst, sem):
        return pltpu.make_async_copy(src, dst, sem)

    def send(src, dst, s, r, peer):
        return pltpu.make_async_remote_copy(src, dst, s, r, device_id=peer, device_id_type=MESH)

    def qkv(i, slot):
        cols = pl.ds(pl.multiple_of(i * hw, hw), hw)
        return [load(w.at[:, cols], wbuf.at[slot, :, k * hw:(k + 1) * hw], wsem.at[slot, k])
                for k, w in enumerate((wq, wk, wv))]

    wo_a = [load(wo.at[:, :wide], wbuf.at[na % SLOTS], wsem.at[na % SLOTS, 0])]
    wo_b = [load(wo.at[:, wide:], wbuf.at[(na + 1) % SLOTS, :, :d - wide], wsem.at[(na + 1) % SLOTS, 0])]

    def unit(e, h, slot):
        w, lo = widths[h], h * wa
        return [load(ue.at[e, :, lo:lo + w], wbuf.at[slot, :, k * w:(k + 1) * w], wsem.at[slot, k])
                for k, ue in enumerate((ue1, ue3))]

    def piece(c, e, slot):
        return load(ue2.at[e, :, pl.ds(pl.multiple_of(c * BLK, BLK), BLK)], ring.at[slot], rsem.at[slot])

    def shared_in(k):
        lo, w = k * wa, min(wa, fs - k * wa)
        n = (n0 + k) % SLOTS
        return [load(ws.at[:, lo:lo + w], wbuf.at[n, :, i * w:(i + 1) * w], wsem.at[n, i])
                for i, ws in enumerate((ws1, ws3))]

    ns = -(-fs // wa)
    n0 = na + 2
    slot_a, slot_b = (n0 + ns) % SLOTS, (n0 + ns + 1) % SLOTS
    rest, tail = fs - d, d - wide
    half = wide - tail
    shared_a = [load(ws2.at[:d, :wide], wbuf.at[slot_a], wsem.at[slot_a, 0])]
    shared_b = [load(ws2.at[:d, wide:], wbuf.at[slot_b, :, :tail], wsem.at[slot_b, 0]),
                load(ws2.at[d:, :half], wbuf.at[slot_b, :rest, tail:], wsem.at[slot_b, 1]),
                load(ws2.at[d:, half:], wbuf.at[slot_b, rest:2 * rest, tail:], wsem.at[slot_b, 2])]

    def start(copies):
        for cp in copies:
            cp.start()

    def wait(copies):
        for cp in copies:
            cp.wait()

    own = [load(h_hbm, h_ref, isem.at[0]), load(tab_hbm, tab_ref, isem.at[1]), load(wr_hbm, wr_ref, isem.at[2])]
    start(own)
    for n in range(SLOTS):
        start(qkv(n, n))
    pts[0] = jnp.concatenate([idx_ref[j] * cap + slot_ref[j] for j in range(top)]
                             + [jnp.full((pts.shape[1] - top, t), -1, jnp.int32)], axis=0)
    ln_a, ln_f, ln_m = (r[...].astype(F32).reshape(1, d) for r in (la_ref, lf_ref, lm_ref))

    barrier = pltpu.get_barrier_semaphore()
    for peer in (core, chip):
        pl.semaphore_signal(barrier, inc=1, device_id=peer, device_id_type=MESH)
    pl.semaphore_wait(barrier, 2)

    rows = t // PIECES
    part = [pl.ds(q * rows, rows) for q in range(PIECES)]
    far = [send(h_hbm.at[part[q]], ub.at[2, part[q]], hs_sem.at[q], hr_sem.at[q], chip) for q in range(PIECES)]
    near = send(h_hbm, ub.at[1], hs_sem.at[PIECES], hr_sem.at[PIECES], core)
    onward = [send(ub.at[2, part[q]], ub.at[3, part[q]], hs_sem.at[PIECES + 1 + q], hr_sem.at[PIECES + 1 + q], core)
              for q in range(PIECES)]
    pfar = send(pts.at[0], pts.at[2], ps_sem.at[0], pr_sem.at[0], chip)
    pnear = send(pts.at[0], pts.at[1], ps_sem.at[1], pr_sem.at[1], core)
    ponward = send(pts.at[2], pts.at[3], ps_sem.at[2], pr_sem.at[2], core)
    start(far)
    near.start()
    wait(own)

    xa[...] = _rms(h_ref[...], ln_a)
    ub[0] = _rms(h_ref[...], ln_m)
    pfar.start()
    pnear.start()

    def heads(i, _):
        slot = lax.rem(i, SLOTS)
        wait(qkv(i, slot))
        z = _dot(xa[...], wbuf[slot])

        @pl.when(i + SLOTS < na)
        def _():
            start(qkv(i + SLOTS, slot))

        for k, nxt in enumerate((wo_a, wo_b, unit(0, 0, (na + 2) % SLOTS))):
            @pl.when(i + SLOTS == na + k)
            def _():
                start(nxt)

        c, s = tab_ref[0], tab_ref[1]
        ok = lax.broadcasted_iota(jnp.int32, (t, t), 0) >= lax.broadcasted_iota(jnp.int32, (t, t), 1)
        outs = []
        for j in range(hw // HEAD):
            qj, kj, vj = (z[:, m * hw + j * HEAD:m * hw + (j + 1) * HEAD] for m in range(3))
            qj = (qj * c + pltpu.roll(qj, HEAD // 2, 1) * s).astype(BF16)
            kj = (kj * c + pltpu.roll(kj, HEAD // 2, 1) * s).astype(BF16)
            sc = lax.dot_general(qj, kj, (((1,), (1,)), ((), ())), preferred_element_type=F32) * HEAD ** -0.5
            sc = jnp.where(ok, sc, -1e30)
            e = jnp.exp(sc - jnp.max(sc, axis=-1, keepdims=True))
            p = (e / jnp.sum(e, axis=-1, keepdims=True)).astype(BF16)
            outs.append(_dot(p, vj.astype(BF16)).astype(BF16))
        sb[:, pl.ds(pl.multiple_of(i * hw, hw), hw)] = jnp.concatenate(outs, axis=-1)
        return 0

    lax.fori_loop(0, na, heads, 0)

    def pass_on(q):
        far[q].wait_recv()
        onward[q].start()

    pfar.wait_recv()
    ponward.start()
    pass_on(0)
    pass_on(1)

    def residual(z, lo):
        a = (h_ref[:, lo:lo + z.shape[1]].astype(F32) + z).astype(BF16)
        xa[:, lo:lo + z.shape[1]] = a
        for c in range(z.shape[1] // BLK):
            base[lo // BLK + c] = a[:, c * BLK:(c + 1) * BLK].astype(F32)

    wait(wo_a)
    residual(_dot(sb[:, :d], wbuf[na % SLOTS]), 0)
    start(unit(0, 1, na % SLOTS))
    wait(wo_b)
    residual(_dot(sb[:, :d], wbuf[(na + 1) % SLOTS, :, :d - wide]), wide)
    start(unit(1, 0, (na + 1) % SLOTS))
    xa[...] = _rms(xa[...], ln_f)
    pass_on(2)
    off = n0 % SLOTS

    def weigh(k):
        pos = jnp.concatenate([pts[k].astype(F32), jnp.zeros((HEAD - pts.shape[1], t), F32)], axis=0).T
        lg = lax.dot_general(ub[k], wr_ref[...], (((1,), (1,)), ((), ())), preferred_element_type=F32)
        lo = lax.broadcasted_iota(jnp.int32, lg.shape, 1).astype(F32) * cap
        picks = []
        for j in range(top):
            off = pos[:, j:j + 1] - lo
            hit = jnp.logical_and(off >= 0, off < cap)
            picks.append(jnp.sum(jnp.where(hit, lg, 0.0), axis=-1, keepdims=True))
        big = functools.reduce(jnp.maximum, picks)
        ex = [jnp.exp(p - big) for p in picks]
        tot = functools.reduce(jnp.add, ex)
        r = (lax.broadcasted_iota(jnp.int32, (t, el * cap), 1) + first).astype(F32)
        c = jnp.zeros(r.shape, F32)
        for j in range(top):
            c += jnp.where(pos[:, j:j + 1] == r, ex[j] / tot, 0.0)
        hi = c.astype(BF16)
        c -= hi.astype(F32)
        mid = c.astype(BF16)
        cm[k, :t] = hi
        cm[k, t:2 * t] = mid
        cm[k, 2 * t:] = (c - mid.astype(F32)).astype(BF16)

    near.wait_recv()
    pnear.wait_recv()
    ub[1] = _rms(ub[1], ln_m)

    def weigh_body(k, _):
        weigh(k)
        return 0

    lax.fori_loop(0, 2, weigh_body, 0)
    pass_on(3)
    for cp in onward:
        cp.wait_send()
    ub[2] = _rms(ub[2], ln_m)
    for cp in onward:
        cp.wait_recv()
    ub[3] = _rms(ub[3], ln_m)
    ponward.wait()
    pfar.wait_send()
    pnear.wait_send()
    near.wait_send()
    for cp in far:
        cp.wait_send()

    def group(g, last):
        for k in range(4):
            r = lax.broadcasted_iota(jnp.int32, (GROUP * cap, t), 0) + (first + g * (GROUP * cap))
            hit = pts[k, 0:1, :] == r
            for j in range(1, top):
                hit = jnp.logical_or(hit, pts[k, j:j + 1, :] == r)
            x = _dot(hit.astype(F32).astype(BF16), ub[k]).astype(BF16)
            for j in range(GROUP):
                x4[j, k * cap:(k + 1) * cap, :] = x[j * cap:(j + 1) * cap]

        @pl.when(g < 2)
        def _():
            weigh(g + 2)

        def ffn_in(j, _):
            e = g * GROUP + j
            for h in range(2):
                slot = lax.rem(2 * e + h + off, SLOTS)
                w = widths[h]
                wait(unit(e, h, slot))
                z = _dot(x4[j], wbuf[slot, :, :2 * w])
                he[e, :, h * wa:h * wa + w] = _silu_mul(z[:, :w], z[:, w:])
                en, hn = e + (h + SLOTS) // 2, (h + SLOTS) % 2

                @pl.when(en < el)
                def _():
                    start(unit(en, hn, slot))

                if h == 0:
                    @pl.when(e == el - 1)
                    def _():
                        for n in range(RING):
                            piece(0, n, n).start()
            return 0

        lax.fori_loop(0, GROUP, ffn_in, 0)
        return last

    lax.fori_loop(0, el // GROUP, group, 0)

    def d2d(c, k):
        p = lax.rem(c, 2)
        return send(sd.at[p, k], rd.at[p, k], sd_sem.at[p, k], rd_sem.at[p, k], core)

    def x2x(c):
        return send(sx.at[c], rx.at[c], sx_sem.at[c], rx_sem.at[c], chip)

    def settle(c):
        d2d(c, 0).wait_recv()
        base[c] += rd[lax.rem(c, 2), 0]

    def chunk(c, _):
        def quad(i, _):
            s0 = GROUP * lax.rem(i, RING // GROUP)
            for k in range(GROUP):
                piece(c, GROUP * i + k, s0 + k).wait()
            for k in range(GROUP):
                e = GROUP * i + k
                y = _dot(he[e], ring[s0 + k]).astype(BF16)
                for b in range(4):
                    ys[b, pl.ds(pl.multiple_of(e * cap, cap), cap), :] = y[b * cap:(b + 1) * cap]
            wrap = (GROUP * i + RING >= el).astype(jnp.int32)

            @pl.when(c + wrap < nc)
            def _():
                for k in range(GROUP):
                    piece(c + wrap, lax.rem(GROUP * i + RING, el) + k, s0 + k).start()
            return 0

        lax.fori_loop(0, el // GROUP, quad, 0)

        for k in range(SLOTS):
            @pl.when(c == k + 1)
            def _():
                start(shared_in(k))

        @pl.when(c >= 2)
        def _():
            for k in range(2):
                d2d(c - 2, k).wait_send()

        @pl.when(c >= 1)
        def _():
            settle(c - 1)

        def total(k):
            z = _dot(cm[k], ys[k])
            return z[:t] + z[t:2 * t] + z[2 * t:]

        sd[lax.rem(c, 2), 1] = total(3)
        d2d(c, 1).start()
        sx[c] = total(2)
        sd[lax.rem(c, 2), 0] = total(1)
        d2d(c, 0).start()
        base[c] += total(0)
        d2d(c, 1).wait_recv()
        sx[c] += rd[lax.rem(c, 2), 1]
        x2x(c).start()
        return 0

    lax.fori_loop(0, nc, chunk, 0)
    settle(nc - 1)
    for c in (nc - 2, nc - 1):
        for k in range(2):
            d2d(c, k).wait_send()

    for k in range(ns):
        wait(shared_in(k))
        w = min(wa, fs - k * wa)
        z = _dot(xa[...], wbuf[(n0 + k) % SLOTS, :, :2 * w])
        sb[:, k * wa:k * wa + w] = _silu_mul(z[:, :w], z[:, w:])
        if k + SLOTS < ns:
            start(shared_in(k + SLOTS))
        elif k + SLOTS == ns:
            start(shared_a)
        elif k + SLOTS == ns + 1:
            start(shared_b)

    def add(z, lo):
        for c in range(z.shape[1] // BLK):
            base[lo // BLK + c] += z[:, c * BLK:(c + 1) * BLK]

    wait(shared_a)
    add(_dot(sb[:, :d], wbuf[slot_a]), 0)
    wait(shared_b)
    add(_dot(sb[:, :d], wbuf[slot_b, :, :tail]), wide)
    add(_dot(sb[:, d:], wbuf[slot_b, :rest, tail:]), 0)
    add(_dot(sb[:, d:], wbuf[slot_b, rest:2 * rest, tail:]), half)

    def put(c):
        return load(ob.at[c], out_hbm.at[:, pl.ds(pl.multiple_of(c * BLK, BLK), BLK)], osem.at[c])

    def finish(c, _):
        x2x(c).wait_recv()
        ob[c] = (base[c] + rx[c]).astype(BF16)
        put(c).start()
        return 0

    lax.fori_loop(0, nc, finish, 0)

    def drain(c, _):
        x2x(c).wait_send()
        put(c).wait()
        return 0

    lax.fori_loop(0, nc, drain, 0)


def solution(mesh):
    rows = P(('dp', 'ep'))
    rep = P()

    def local(h0, idx, slot, ln_attn, wq, wk, wv, wo, ln_ffn, ws1, ws3, ws2, ln_moe, wr, ue1, ue3, ue2):
        b, s, d = h0.shape
        top = idx.shape[-1]
        el, _, fe = ue1.shape
        fs = ws1.shape[1]
        t = b * s
        cap = CAP_FACTOR * t * top // (el * mesh.shape['ep'])
        nc = d // BLK
        wide = 2 * ((fe // 2 + HEAD - 1) // HEAD * HEAD)
        hbm = pl.BlockSpec(memory_space=pl.ANY)
        vmem = pl.BlockSpec(memory_space=pltpu.VMEM)
        dma = pltpu.SemaphoreType.DMA
        out = pl.pallas_call(
            functools.partial(_layer, el, cap, top),
            in_specs=[vmem] * 5 + [hbm] * 13,
            out_specs=hbm,
            out_shape=jax.ShapeDtypeStruct((t, d), BF16),
            scratch_shapes=[
                pltpu.VMEM((t, d), BF16), pltpu.VMEM((2, s, HEAD), F32), pltpu.VMEM((wr.shape[1], d), BF16),
                pltpu.VMEM((SLOTS, d, wide), BF16), pltpu.VMEM((RING, fe, BLK), BF16), pltpu.VMEM((el, 4 * cap, fe), BF16),
                pltpu.VMEM((4, t, d), BF16), pltpu.VMEM((t, d), BF16), pltpu.VMEM((t, fs), BF16),
                pltpu.VMEM((GROUP, 4 * cap, d), BF16), pltpu.VMEM((4, el * cap, BLK), BF16),
                pltpu.VMEM((4, 3 * t, el * cap), BF16), pltpu.VMEM((4, 8, t), jnp.int32),
                pltpu.VMEM((2, 2, t, BLK), F32), pltpu.VMEM((2, 2, t, BLK), F32),
                pltpu.VMEM((nc, t, BLK), F32), pltpu.VMEM((nc, t, BLK), F32), pltpu.VMEM((nc, t, BLK), F32),
                pltpu.VMEM((nc, t, BLK), BF16),
                dma((3,)), dma((SLOTS, 3)), dma((RING,)), dma((nc,)), dma((2 * PIECES + 1,)), dma((2 * PIECES + 1,)), dma((3,)), dma((3,)),
                dma((2, 2)), dma((2, 2)), dma((nc,)), dma((nc,)),
            ],
            compiler_params=pltpu.CompilerParams(collective_id=0, has_side_effects=True, vmem_limit_bytes=67043328),
            name='layer',
        )(idx.reshape(t, 1, top).transpose(2, 1, 0), slot.reshape(t, 1, top).transpose(2, 1, 0), ln_attn, ln_ffn, ln_moe,
          h0.reshape(t, d), jnp.asarray(_tables(s)), wr.T, wq, wk, wv, wo, ws1, ws3, ws2, ue1, ue3, ue2)
        return out.reshape(b, s, d)

    specs = (rows, rows, rows) + (rep,) * 11 + (P('ep'), P('ep'), P('ep'))
    return jax.shard_map(local, mesh=mesh, in_specs=specs, out_specs=rows, check_vma=False)
```

```python
import functools

import jax
import jax.numpy as jnp
import numpy as np
from jax import lax
from jax.experimental import pallas as pl
from jax.experimental.pallas import tpu as pltpu
from jax.sharding import PartitionSpec as P

HEAD = 128
EPS = 1e-6
CAP_FACTOR = 2
BLK = 256
SLOTS = 4
GROUP = 4
PIECES = 4
HOLD = 4
MESH = pl.DeviceIdType.MESH
F32, BF16 = jnp.float32, jnp.bfloat16


def _dot(a, b):
    return jnp.dot(a, b, preferred_element_type=F32)


def _rms(x, w):
    xf = x.astype(F32)
    r = lax.rsqrt(jnp.mean(xf * xf, axis=-1, keepdims=True) + EPS)
    return (xf * r * w).astype(BF16)


def _silu_mul(h1, h3):
    return (h1 * jax.nn.sigmoid(h1) * h3).astype(BF16)


def _tables(s):
    half = HEAD // 2
    freq = np.float32(10000.0) ** (-np.arange(half, dtype=np.float32) / np.float32(half))
    ang = np.arange(s, dtype=np.float32)[:, None] * freq[None, :]
    c, sn = np.cos(ang), np.sin(ang)
    return np.stack([np.concatenate([c, c], axis=-1), np.concatenate([-sn, sn], axis=-1)]).astype(np.float32)


def _layer(el, cap, top, idx_ref, slot_ref, la_ref, lf_ref, lm_ref, h_hbm, tab_hbm, wr_hbm, wq, wk, wv, wo, ws1, ws3, ws2, ue1, ue3, ue2, out_hbm,
           h_ref, tab_ref, wr_ref, wbuf, he, ub, xa, sb, x4, ys, cm, pts, sd, rd, sx, rx, base,
           isem, wsem, osem, hs_sem, hr_sem, ps_sem, pr_sem, sd_sem, rd_sem, sx_sem, rx_sem):
    me = lax.axis_index('ep')
    dp = lax.axis_index('dp')
    core = (dp, me + 1 - 2 * lax.rem(me, 2))
    chip = (dp, lax.rem(me + 2, 4))
    t, d = h_ref.shape
    fe, fs = ue1.shape[2], ws1.shape[1]
    wide = wbuf.shape[2]
    wa = wide // 2
    widths = (wa, fe - wa)
    nc = d // BLK
    hw = wide // 3
    na = d // hw
    first = me * (el * cap)

    def load(src, dst, sem):
        return pltpu.make_async_copy(src, dst, sem)

    def send(src, dst, s, r, peer):
        return pltpu.make_async_remote_copy(src, dst, s, r, device_id=peer, device_id_type=MESH)

    def qkv(i, slot):
        cols = pl.ds(pl.multiple_of(i * hw, hw), hw)
        return [load(w.at[:, cols], wbuf.at[slot, :, k * hw:(k + 1) * hw], wsem.at[slot, k])
                for k, w in enumerate((wq, wk, wv))]

    wo_a = [load(wo.at[:, :wide], wbuf.at[na % SLOTS], wsem.at[na % SLOTS, 0])]
    wo_b = [load(wo.at[:, wide:], wbuf.at[(na + 1) % SLOTS, :, :d - wide], wsem.at[(na + 1) % SLOTS, 0])]

    def unit(e, h, slot):
        w, lo = widths[h], h * wa
        return [load(ue.at[e, :, lo:lo + w], wbuf.at[slot, :, k * w:(k + 1) * w], wsem.at[slot, k])
                for k, ue in enumerate((ue1, ue3))]

    def pieces(c, i, slot):
        cols = pl.ds(pl.multiple_of(c * BLK, BLK), BLK)
        return [load(ue2.at[GROUP * i + k, :, cols], wbuf.at[slot, :fe, k * BLK:(k + 1) * BLK], wsem.at[slot, k])
                for k in range(GROUP)]

    def shared_in(k):
        lo, w = k * wa, min(wa, fs - k * wa)
        n = (n0 + k) % SLOTS
        return [load(ws.at[:, lo:lo + w], wbuf.at[n, :, i * w:(i + 1) * w], wsem.at[n, i])
                for i, ws in enumerate((ws1, ws3))]

    ns = -(-fs // wa)
    up0 = na + 2
    down0 = up0 + 2 * el
    n0 = down0 + nc * (el // GROUP)
    slot_a, slot_b = (n0 + ns) % SLOTS, (n0 + ns + 1) % SLOTS
    rest, tail = fs - d, d - wide
    half = wide - tail
    shared_a = [load(ws2.at[:d, :wide], wbuf.at[slot_a], wsem.at[slot_a, 0])]
    shared_b = [load(ws2.at[:d, wide:], wbuf.at[slot_b, :, :tail], wsem.at[slot_b, 0]),
                load(ws2.at[d:, :half], wbuf.at[slot_b, :rest, tail:], wsem.at[slot_b, 1]),
                load(ws2.at[d:, half:], wbuf.at[slot_b, rest:2 * rest, tail:], wsem.at[slot_b, 2])]

    def start(copies):
        for cp in copies:
            cp.start()

    def wait(copies):
        for cp in copies:
            cp.wait()

    own = [load(h_hbm, h_ref, isem.at[0]), load(tab_hbm, tab_ref, isem.at[1]), load(wr_hbm, wr_ref, isem.at[2])]
    start(own)
    for n in range(SLOTS):
        start(qkv(n, n))
    pts[0] = jnp.concatenate([idx_ref[j] * cap + slot_ref[j] for j in range(top)]
                             + [jnp.full((pts.shape[1] - top, t), -1, jnp.int32)], axis=0)
    ln_a, ln_f, ln_m = (r[...].astype(F32).reshape(1, d) for r in (la_ref, lf_ref, lm_ref))

    barrier = pltpu.get_barrier_semaphore()
    for peer in (core, chip):
        pl.semaphore_signal(barrier, inc=1, device_id=peer, device_id_type=MESH)
    pl.semaphore_wait(barrier, 2)

    rows = t // PIECES
    part = [pl.ds(q * rows, rows) for q in range(PIECES)]
    far = [send(h_hbm.at[part[q]], ub.at[2, part[q]], hs_sem.at[q], hr_sem.at[q], chip) for q in range(PIECES)]
    near = send(h_hbm, ub.at[1], hs_sem.at[PIECES], hr_sem.at[PIECES], core)
    onward = [send(ub.at[2, part[q]], ub.at[3, part[q]], hs_sem.at[PIECES + 1 + q], hr_sem.at[PIECES + 1 + q], core)
              for q in range(PIECES)]
    pfar = send(pts.at[0], pts.at[2], ps_sem.at[0], pr_sem.at[0], chip)
    pnear = send(pts.at[0], pts.at[1], ps_sem.at[1], pr_sem.at[1], core)
    ponward = send(pts.at[2], pts.at[3], ps_sem.at[2], pr_sem.at[2], core)
    start(far)
    near.start()
    wait(own)

    xa[...] = _rms(h_ref[...], ln_a)
    ub[0] = _rms(h_ref[...], ln_m)
    pfar.start()
    pnear.start()

    def heads(i, _):
        slot = lax.rem(i, SLOTS)
        wait(qkv(i, slot))
        z = _dot(xa[...], wbuf[slot])

        for k, nxt in enumerate((wo_a, wo_b, unit(0, 0, up0 % SLOTS), unit(0, 1, (up0 + 1) % SLOTS))):
            @pl.when(i == k)
            def _():
                start(nxt)

        c, s = tab_ref[0], tab_ref[1]
        ok = lax.broadcasted_iota(jnp.int32, (t, t), 0) >= lax.broadcasted_iota(jnp.int32, (t, t), 1)
        outs = []
        for j in range(hw // HEAD):
            qj, kj, vj = (z[:, m * hw + j * HEAD:m * hw + (j + 1) * HEAD] for m in range(3))
            qj = (qj * c + pltpu.roll(qj, HEAD // 2, 1) * s).astype(BF16)
            kj = (kj * c + pltpu.roll(kj, HEAD // 2, 1) * s).astype(BF16)
            sc = lax.dot_general(qj, kj, (((1,), (1,)), ((), ())), preferred_element_type=F32) * HEAD ** -0.5
            sc = jnp.where(ok, sc, -1e30)
            e = jnp.exp(sc - jnp.max(sc, axis=-1, keepdims=True))
            p = (e / jnp.sum(e, axis=-1, keepdims=True)).astype(BF16)
            outs.append(_dot(p, vj.astype(BF16)).astype(BF16))
        sb[:, pl.ds(pl.multiple_of(i * hw, hw), hw)] = jnp.concatenate(outs, axis=-1)
        return 0

    lax.fori_loop(0, na, heads, 0)

    def pass_on(q):
        far[q].wait_recv()
        onward[q].start()

    pfar.wait_recv()
    ponward.start()
    pass_on(0)
    pass_on(1)

    def residual(z, lo):
        a = (h_ref[:, lo:lo + z.shape[1]].astype(F32) + z).astype(BF16)
        xa[:, lo:lo + z.shape[1]] = a
        for c in range(z.shape[1] // BLK):
            base[lo // BLK + c] = a[:, c * BLK:(c + 1) * BLK].astype(F32)

    wait(wo_a)
    residual(_dot(sb[:, :d], wbuf[na % SLOTS]), 0)
    start(unit(1, 0, na % SLOTS))
    wait(wo_b)
    residual(_dot(sb[:, :d], wbuf[(na + 1) % SLOTS, :, :d - wide]), wide)
    start(unit(1, 1, (na + 1) % SLOTS))
    xa[...] = _rms(xa[...], ln_f)
    pass_on(2)
    off = up0 % SLOTS

    def weigh(k):
        pos = jnp.concatenate([pts[k].astype(F32), jnp.zeros((HEAD - pts.shape[1], t), F32)], axis=0).T
        lg = lax.dot_general(ub[k], wr_ref[...], (((1,), (1,)), ((), ())), preferred_element_type=F32)
        lo = lax.broadcasted_iota(jnp.int32, lg.shape, 1).astype(F32) * cap
        picks = []
        for j in range(top):
            off = pos[:, j:j + 1] - lo
            hit = jnp.logical_and(off >= 0, off < cap)
            picks.append(jnp.sum(jnp.where(hit, lg, 0.0), axis=-1, keepdims=True))
        big = functools.reduce(jnp.maximum, picks)
        ex = [jnp.exp(p - big) for p in picks]
        tot = functools.reduce(jnp.add, ex)
        r = (lax.broadcasted_iota(jnp.int32, (t, el * cap), 1) + first).astype(F32)
        c = jnp.zeros(r.shape, F32)
        for j in range(top):
            c += jnp.where(pos[:, j:j + 1] == r, ex[j] / tot, 0.0)
        hi = c.astype(BF16)
        c -= hi.astype(F32)
        mid = c.astype(BF16)
        cm[k, :t] = hi
        cm[k, t:2 * t] = mid
        cm[k, 2 * t:] = (c - mid.astype(F32)).astype(BF16)

    near.wait_recv()
    pnear.wait_recv()
    ub[1] = _rms(ub[1], ln_m)

    def weigh_body(k, _):
        weigh(k)
        return 0

    lax.fori_loop(0, 2, weigh_body, 0)
    pass_on(3)
    for cp in onward:
        cp.wait_send()
    ub[2] = _rms(ub[2], ln_m)
    for cp in onward:
        cp.wait_recv()
    ub[3] = _rms(ub[3], ln_m)
    ponward.wait()
    pfar.wait_send()
    pnear.wait_send()
    near.wait_send()
    for cp in far:
        cp.wait_send()

    def group(g, last):
        for k in range(4):
            r = lax.broadcasted_iota(jnp.int32, (GROUP * cap, t), 0) + (first + g * (GROUP * cap))
            hit = pts[k, 0:1, :] == r
            for j in range(1, top):
                hit = jnp.logical_or(hit, pts[k, j:j + 1, :] == r)
            x = _dot(hit.astype(F32).astype(BF16), ub[k]).astype(BF16)
            for j in range(GROUP):
                x4[j, k * cap:(k + 1) * cap, :] = x[j * cap:(j + 1) * cap]

        @pl.when(g < 2)
        def _():
            weigh(g + 2)

        def ffn_in(j, _):
            e = g * GROUP + j
            for h in range(2):
                slot = lax.rem(2 * e + h + off, SLOTS)
                w = widths[h]
                wait(unit(e, h, slot))
                z = _dot(x4[j], wbuf[slot, :, :2 * w])
                he[e, :, h * wa:h * wa + w] = _silu_mul(z[:, :w], z[:, w:])

                @pl.when(e + 2 < el)
                def _():
                    start(unit(e + 2, h, slot))

                @pl.when(e + 2 >= el)
                def _():
                    start(pieces(0, 2 * (e + 2 - el) + h, slot))
            return 0

        lax.fori_loop(0, GROUP, ffn_in, 0)
        return last

    lax.fori_loop(0, el // GROUP, group, 0)

    def d2d(c, k):
        p = lax.rem(c, 2)
        return send(sd.at[p, k], rd.at[p, k], sd_sem.at[p, k], rd_sem.at[p, k], core)

    def x2x(c):
        p = lax.rem(c, HOLD)
        return send(sx.at[p], rx.at[c], sx_sem.at[p], rx_sem.at[c], chip)

    def settle(c):
        d2d(c, 0).wait_recv()
        base[c] += rd[lax.rem(c, 2), 0]

    def chunk(c, _):
        def quad(i, _):
            slot = lax.rem(i + down0, SLOTS)
            wait(pieces(c, i, slot))
            for k in range(GROUP):
                e = GROUP * i + k
                y = _dot(he[e], wbuf[slot, :fe, k * BLK:(k + 1) * BLK]).astype(BF16)
                for b in range(4):
                    ys[b, pl.ds(pl.multiple_of(e * cap, cap), cap), :] = y[b * cap:(b + 1) * cap]

            @pl.when(c + 1 < nc)
            def _():
                start(pieces(c + 1, i, slot))

            for k in range(ns):
                @pl.when(jnp.logical_and(c + 1 == nc, i == k))
                def _():
                    start(shared_in(k))
            return 0

        lax.fori_loop(0, el // GROUP, quad, 0)

        @pl.when(c >= 2)
        def _():
            for k in range(2):
                d2d(c - 2, k).wait_send()

        @pl.when(c >= 1)
        def _():
            settle(c - 1)

        def total(k):
            z = _dot(cm[k], ys[k])
            return z[:t] + z[t:2 * t] + z[2 * t:]

        sd[lax.rem(c, 2), 1] = total(3)
        d2d(c, 1).start()

        @pl.when(c >= HOLD)
        def _():
            x2x(c - HOLD).wait_send()

        sx[lax.rem(c, HOLD)] = total(2)
        sd[lax.rem(c, 2), 0] = total(1)
        d2d(c, 0).start()
        base[c] += total(0)
        d2d(c, 1).wait_recv()
        sx[lax.rem(c, HOLD)] += rd[lax.rem(c, 2), 1]
        x2x(c).start()
        return 0

    lax.fori_loop(0, nc, chunk, 0)
    settle(nc - 1)
    for c in (nc - 2, nc - 1):
        for k in range(2):
            d2d(c, k).wait_send()

    for k in range(ns):
        wait(shared_in(k))
        w = min(wa, fs - k * wa)
        z = _dot(xa[...], wbuf[(n0 + k) % SLOTS, :, :2 * w])
        sb[:, k * wa:k * wa + w] = _silu_mul(z[:, :w], z[:, w:])
        if k == 0:
            start(shared_a)
        elif k == 1:
            start(shared_b)

    def add(z, lo):
        for c in range(z.shape[1] // BLK):
            base[lo // BLK + c] += z[:, c * BLK:(c + 1) * BLK]

    wait(shared_a)
    add(_dot(sb[:, :d], wbuf[slot_a]), 0)
    wait(shared_b)
    add(_dot(sb[:, :d], wbuf[slot_b, :, :tail]), wide)
    add(_dot(sb[:, d:], wbuf[slot_b, :rest, tail:]), 0)
    add(_dot(sb[:, d:], wbuf[slot_b, rest:2 * rest, tail:]), half)

    def put(c):
        cols = pl.ds(pl.multiple_of(c * BLK, BLK), BLK)
        return load(xa.at[:, cols], out_hbm.at[:, cols], osem.at[c])

    def finish(c, _):
        x2x(c).wait_recv()
        xa[:, pl.ds(pl.multiple_of(c * BLK, BLK), BLK)] = (base[c] + rx[c]).astype(BF16)
        put(c).start()
        return 0

    lax.fori_loop(0, nc, finish, 0)
    for c in range(nc - HOLD, nc):
        x2x(c).wait_send()

    def drain(c, _):
        put(c).wait()
        return 0

    lax.fori_loop(0, nc, drain, 0)


def solution(mesh):
    rows = P(('dp', 'ep'))
    rep = P()

    def local(h0, idx, slot, ln_attn, wq, wk, wv, wo, ln_ffn, ws1, ws3, ws2, ln_moe, wr, ue1, ue3, ue2):
        b, s, d = h0.shape
        top = idx.shape[-1]
        el, _, fe = ue1.shape
        fs = ws1.shape[1]
        t = b * s
        cap = CAP_FACTOR * t * top // (el * mesh.shape['ep'])
        nc = d // BLK
        wide = 2 * ((fe // 2 + HEAD - 1) // HEAD * HEAD)
        hbm = pl.BlockSpec(memory_space=pl.ANY)
        vmem = pl.BlockSpec(memory_space=pltpu.VMEM)
        dma = pltpu.SemaphoreType.DMA
        out = pl.pallas_call(
            functools.partial(_layer, el, cap, top),
            in_specs=[vmem] * 5 + [hbm] * 13,
            out_specs=hbm,
            out_shape=jax.ShapeDtypeStruct((t, d), BF16),
            scratch_shapes=[
                pltpu.VMEM((t, d), BF16), pltpu.VMEM((2, s, HEAD), F32), pltpu.VMEM((wr.shape[1], d), BF16),
                pltpu.VMEM((SLOTS, d, wide), BF16), pltpu.VMEM((el, 4 * cap, fe), BF16),
                pltpu.VMEM((4, t, d), BF16), pltpu.VMEM((t, d), BF16), pltpu.VMEM((t, fs), BF16),
                pltpu.VMEM((GROUP, 4 * cap, d), BF16), pltpu.VMEM((4, el * cap, BLK), BF16),
                pltpu.VMEM((4, 3 * t, el * cap), BF16), pltpu.VMEM((4, 8, t), jnp.int32),
                pltpu.VMEM((2, 2, t, BLK), F32), pltpu.VMEM((2, 2, t, BLK), F32),
                pltpu.VMEM((HOLD, t, BLK), F32), pltpu.VMEM((nc, t, BLK), F32), pltpu.VMEM((nc, t, BLK), F32),
                dma((3,)), dma((SLOTS, GROUP)), dma((nc,)), dma((2 * PIECES + 1,)), dma((2 * PIECES + 1,)), dma((3,)), dma((3,)),
                dma((2, 2)), dma((2, 2)), dma((HOLD,)), dma((nc,)),
            ],
            compiler_params=pltpu.CompilerParams(collective_id=0, has_side_effects=True, vmem_limit_bytes=67043328),
            name='layer',
        )(idx.reshape(t, 1, top).transpose(2, 1, 0), slot.reshape(t, 1, top).transpose(2, 1, 0), ln_attn, ln_ffn, ln_moe,
          h0.reshape(t, d), jnp.asarray(_tables(s)), wr.T, wq, wk, wv, wo, ws1, ws3, ws2, ue1, ue3, ue2)
        return out.reshape(b, s, d)

    specs = (rows, rows, rows) + (rep,) * 11 + (P('ep'), P('ep'), P('ep'))
    return jax.shard_map(local, mesh=mesh, in_specs=specs, out_specs=rows, check_vma=False)
```

```python
import functools

import jax
import jax.numpy as jnp
import numpy as np
from jax import lax
from jax.experimental import pallas as pl
from jax.experimental.pallas import tpu as pltpu
from jax.sharding import PartitionSpec as P

HEAD = 128
EPS = 1e-6
CAP_FACTOR = 2
BLK = 256
SLOTS = 4
GROUP = 4
PIECES = 4
HOLD = 4
MESH = pl.DeviceIdType.MESH
F32, BF16 = jnp.float32, jnp.bfloat16


def _dot(a, b):
    return jnp.dot(a, b, preferred_element_type=F32)


def _rms(x, w):
    xf = x.astype(F32)
    r = lax.rsqrt(jnp.mean(xf * xf, axis=-1, keepdims=True) + EPS)
    return (xf * r * w).astype(BF16)


def _silu_mul(h1, h3):
    return (h1 * jax.nn.sigmoid(h1) * h3).astype(BF16)


def _tables(s):
    half = HEAD // 2
    freq = np.float32(10000.0) ** (-np.arange(half, dtype=np.float32) / np.float32(half))
    ang = np.arange(s, dtype=np.float32)[:, None] * freq[None, :]
    c, sn = np.cos(ang), np.sin(ang)
    return np.stack([np.concatenate([c, c], axis=-1), np.concatenate([-sn, sn], axis=-1)]).astype(np.float32)


def _layer(el, cap, top, idx_ref, slot_ref, la_ref, lf_ref, lm_ref, h_hbm, tab_hbm, wr_hbm, wq, wk, wv, wo, ws1, ws3, ws2, ue1, ue3, ue2, out_hbm,
           h_ref, tab_ref, wr_ref, wbuf, he, ub, xa, sb, x4, ys, cm, pts, sd, rd, sx, rx, base,
           isem, wsem, osem, hs_sem, hr_sem, ps_sem, pr_sem, sd_sem, rd_sem, sx_sem, rx_sem):
    me = lax.axis_index('ep')
    dp = lax.axis_index('dp')
    core = (dp, me + 1 - 2 * lax.rem(me, 2))
    chip = (dp, lax.rem(me + 2, 4))
    t, d = h_ref.shape
    fe, fs = ue1.shape[2], ws1.shape[1]
    wide = wbuf.shape[2]
    wa = wide // 2
    widths = (wa, fe - wa)
    nc = d // BLK
    hw = wide // 3
    na = d // hw
    first = me * (el * cap)

    def load(src, dst, sem):
        return pltpu.make_async_copy(src, dst, sem)

    def send(src, dst, s, r, peer):
        return pltpu.make_async_remote_copy(src, dst, s, r, device_id=peer, device_id_type=MESH)

    def qkv(i, slot):
        cols = pl.ds(pl.multiple_of(i * hw, hw), hw)
        return [load(w.at[:, cols], wbuf.at[slot, :, k * hw:(k + 1) * hw], wsem.at[slot, k])
                for k, w in enumerate((wq, wk, wv))]

    wo_a = [load(wo.at[:, :wide], wbuf.at[na % SLOTS], wsem.at[na % SLOTS, 0])]
    wo_b = [load(wo.at[:, wide:], wbuf.at[(na + 1) % SLOTS, :, :d - wide], wsem.at[(na + 1) % SLOTS, 0])]

    def unit(e, h, slot):
        w, lo = widths[h], h * wa
        return [load(ue.at[e, :, lo:lo + w], wbuf.at[slot, :, k * w:(k + 1) * w], wsem.at[slot, k])
                for k, ue in enumerate((ue1, ue3))]

    def pieces(c, i, slot):
        cols = pl.ds(pl.multiple_of(c * BLK, BLK), BLK)
        return [load(ue2.at[GROUP * i + k, :, cols], wbuf.at[slot, :fe, k * BLK:(k + 1) * BLK], wsem.at[slot, k])
                for k in range(GROUP)]

    def shared_in(k):
        lo, w = k * wa, min(wa, fs - k * wa)
        n = (n0 + k) % SLOTS
        return [load(ws.at[:, lo:lo + w], wbuf.at[n, :, i * w:(i + 1) * w], wsem.at[n, i])
                for i, ws in enumerate((ws1, ws3))]

    ns = -(-fs // wa)
    up0 = na + 2
    down0 = up0 + 2 * el
    n0 = down0 + nc * (el // GROUP)
    slot_a, slot_b = (n0 + ns) % SLOTS, (n0 + ns + 1) % SLOTS
    rest, tail = fs - d, d - wide
    half = wide - tail
    shared_a = [load(ws2.at[:d, :wide], wbuf.at[slot_a], wsem.at[slot_a, 0])]
    shared_b = [load(ws2.at[:d, wide:], wbuf.at[slot_b, :, :tail], wsem.at[slot_b, 0]),
                load(ws2.at[d:, :half], wbuf.at[slot_b, :rest, tail:], wsem.at[slot_b, 1]),
                load(ws2.at[d:, half:], wbuf.at[slot_b, rest:2 * rest, tail:], wsem.at[slot_b, 2])]

    def start(copies):
        for cp in copies:
            cp.start()

    def wait(copies):
        for cp in copies:
            cp.wait()

    own = [load(h_hbm, h_ref, isem.at[0]), load(tab_hbm, tab_ref, isem.at[1]), load(wr_hbm, wr_ref, isem.at[2])]
    start(own)
    for n in range(SLOTS):
        start(qkv(n, n))
    pts[0] = jnp.concatenate([idx_ref[j] * cap + slot_ref[j] for j in range(top)]
                             + [jnp.full((pts.shape[1] - top, t), -1, jnp.int32)], axis=0)
    ln_a, ln_f, ln_m = (r[...].astype(F32).reshape(1, d) for r in (la_ref, lf_ref, lm_ref))

    barrier = pltpu.get_barrier_semaphore()
    for peer in (core, chip):
        pl.semaphore_signal(barrier, inc=1, device_id=peer, device_id_type=MESH)
    pl.semaphore_wait(barrier, 2)

    rows = t // PIECES
    part = [pl.ds(q * rows, rows) for q in range(PIECES)]
    far = [send(h_hbm.at[part[q]], ub.at[2, part[q]], hs_sem.at[q], hr_sem.at[q], chip) for q in range(PIECES)]
    near = send(h_hbm, ub.at[1], hs_sem.at[PIECES], hr_sem.at[PIECES], core)
    onward = [send(ub.at[2, part[q]], ub.at[3, part[q]], hs_sem.at[PIECES + 1 + q], hr_sem.at[PIECES + 1 + q], core)
              for q in range(PIECES)]
    pfar = send(pts.at[0], pts.at[2], ps_sem.at[0], pr_sem.at[0], chip)
    pnear = send(pts.at[0], pts.at[1], ps_sem.at[1], pr_sem.at[1], core)
    ponward = send(pts.at[2], pts.at[3], ps_sem.at[2], pr_sem.at[2], core)
    start(far)
    near.start()
    wait(own)

    xa[...] = _rms(h_ref[...], ln_a)
    ub[0] = _rms(h_ref[...], ln_m)
    pfar.start()
    pnear.start()

    def heads(i, _):
        slot = lax.rem(i, SLOTS)
        wait(qkv(i, slot))
        z = _dot(xa[...], wbuf[slot])

        for k, nxt in enumerate((wo_a, wo_b, unit(0, 0, up0 % SLOTS), unit(0, 1, (up0 + 1) % SLOTS))):
            @pl.when(i == k)
            def _():
                start(nxt)

        c, s = tab_ref[0], tab_ref[1]
        ok = lax.broadcasted_iota(jnp.int32, (t, t), 0) >= lax.broadcasted_iota(jnp.int32, (t, t), 1)
        outs = []
        for j in range(hw // HEAD):
            qj, kj, vj = (z[:, m * hw + j * HEAD:m * hw + (j + 1) * HEAD] for m in range(3))
            qj = (qj * c + pltpu.roll(qj, HEAD // 2, 1) * s).astype(BF16)
            kj = (kj * c + pltpu.roll(kj, HEAD // 2, 1) * s).astype(BF16)
            sc = lax.dot_general(qj, kj, (((1,), (1,)), ((), ())), preferred_element_type=F32) * HEAD ** -0.5
            sc = jnp.where(ok, sc, -1e30)
            e = jnp.exp(sc - jnp.max(sc, axis=-1, keepdims=True))
            p = (e / jnp.sum(e, axis=-1, keepdims=True)).astype(BF16)
            outs.append(_dot(p, vj.astype(BF16)).astype(BF16))
        sb[:, pl.ds(pl.multiple_of(i * hw, hw), hw)] = jnp.concatenate(outs, axis=-1)
        return 0

    lax.fori_loop(0, na, heads, 0)

    def pass_on(q):
        far[q].wait_recv()
        onward[q].start()

    pfar.wait_recv()
    ponward.start()
    pass_on(0)
    pass_on(1)

    def residual(z, lo):
        a = (h_ref[:, lo:lo + z.shape[1]].astype(F32) + z).astype(BF16)
        xa[:, lo:lo + z.shape[1]] = a
        for c in range(z.shape[1] // BLK):
            base[lo // BLK + c] = a[:, c * BLK:(c + 1) * BLK].astype(F32)

    wait(wo_a)
    residual(_dot(sb[:, :d], wbuf[na % SLOTS]), 0)
    start(unit(1, 0, na % SLOTS))
    wait(wo_b)
    residual(_dot(sb[:, :d], wbuf[(na + 1) % SLOTS, :, :d - wide]), wide)
    start(unit(1, 1, (na + 1) % SLOTS))
    xa[...] = _rms(xa[...], ln_f)
    pass_on(2)
    off = up0 % SLOTS

    def weigh(k):
        pos = jnp.concatenate([pts[k].astype(F32), jnp.zeros((HEAD - pts.shape[1], t), F32)], axis=0).T
        lg = lax.dot_general(ub[k], wr_ref[...], (((1,), (1,)), ((), ())), preferred_element_type=F32)
        lo = lax.broadcasted_iota(jnp.int32, lg.shape, 1).astype(F32) * cap
        picks = []
        for j in range(top):
            off = pos[:, j:j + 1] - lo
            hit = jnp.logical_and(off >= 0, off < cap)
            picks.append(jnp.sum(jnp.where(hit, lg, 0.0), axis=-1, keepdims=True))
        big = functools.reduce(jnp.maximum, picks)
        ex = [jnp.exp(p - big) for p in picks]
        tot = functools.reduce(jnp.add, ex)
        r = (lax.broadcasted_iota(jnp.int32, (t, el * cap), 1) + first).astype(F32)
        c = jnp.zeros(r.shape, F32)
        for j in range(top):
            c += jnp.where(pos[:, j:j + 1] == r, ex[j] / tot, 0.0)
        hi = c.astype(BF16)
        c -= hi.astype(F32)
        mid = c.astype(BF16)
        cm[k, :t] = hi
        cm[k, t:2 * t] = mid
        cm[k, 2 * t:] = (c - mid.astype(F32)).astype(BF16)

    near.wait_recv()
    pnear.wait_recv()
    ub[1] = _rms(ub[1], ln_m)

    pass_on(3)
    for cp in onward:
        cp.wait_send()
    ub[2] = _rms(ub[2], ln_m)
    for cp in onward:
        cp.wait_recv()
    ub[3] = _rms(ub[3], ln_m)
    ponward.wait()
    pfar.wait_send()
    pnear.wait_send()
    near.wait_send()
    for cp in far:
        cp.wait_send()

    def group(g, last):
        weigh(g)
        for k in range(4):
            r = lax.broadcasted_iota(jnp.int32, (GROUP * cap, t), 0) + (first + g * (GROUP * cap))
            hit = pts[k, 0:1, :] == r
            for j in range(1, top):
                hit = jnp.logical_or(hit, pts[k, j:j + 1, :] == r)
            x = _dot(hit.astype(F32).astype(BF16), ub[k]).astype(BF16)
            for j in range(GROUP):
                x4[j, k * cap:(k + 1) * cap, :] = x[j * cap:(j + 1) * cap]

        def ffn_in(j, _):
            e = g * GROUP + j
            for h in range(2):
                slot = lax.rem(2 * e + h + off, SLOTS)
                w = widths[h]
                wait(unit(e, h, slot))
                z = _dot(x4[j], wbuf[slot, :, :2 * w])
                he[e, :, h * wa:h * wa + w] = _silu_mul(z[:, :w], z[:, w:])

                @pl.when(e + 2 < el)
                def _():
                    start(unit(e + 2, h, slot))

                @pl.when(e + 2 >= el)
                def _():
                    start(pieces(0, 2 * (e + 2 - el) + h, slot))
            return 0

        lax.fori_loop(0, GROUP, ffn_in, 0)
        return last

    lax.fori_loop(0, el // GROUP, group, 0)

    def d2d(c, k):
        p = lax.rem(c, 2)
        return send(sd.at[p, k], rd.at[p, k], sd_sem.at[p, k], rd_sem.at[p, k], core)

    def x2x(c):
        p = lax.rem(c, HOLD)
        return send(sx.at[p], rx.at[c], sx_sem.at[p], rx_sem.at[c], chip)

    def settle(c):
        d2d(c, 0).wait_recv()
        base[c] += rd[lax.rem(c, 2), 0]

    def chunk(c, _):
        def duo(m, _):
            steps = [(2 * m + q, lax.rem(2 * m + q + down0, SLOTS)) for q in range(2)]
            for i, slot in steps:
                wait(pieces(c, i, slot))
            for i, slot in steps:
                for k in range(GROUP):
                    e = GROUP * i + k
                    y = _dot(he[e], wbuf[slot, :fe, k * BLK:(k + 1) * BLK]).astype(BF16)
                    for b in range(4):
                        ys[b, pl.ds(pl.multiple_of(e * cap, cap), cap), :] = y[b * cap:(b + 1) * cap]

            @pl.when(c + 1 < nc)
            def _():
                for i, slot in steps:
                    start(pieces(c + 1, i, slot))

            for k in range(ns // 2):
                @pl.when(jnp.logical_and(c + 1 == nc, m == k))
                def _():
                    start(shared_in(2 * k))
                    start(shared_in(2 * k + 1))
            return 0

        lax.fori_loop(0, el // GROUP // 2, duo, 0)

        @pl.when(c >= 2)
        def _():
            for k in range(2):
                d2d(c - 2, k).wait_send()

        @pl.when(c >= 1)
        def _():
            settle(c - 1)

        def total(k):
            z = _dot(cm[k], ys[k])
            return z[:t] + z[t:2 * t] + z[2 * t:]

        sd[lax.rem(c, 2), 1] = total(3)
        d2d(c, 1).start()

        @pl.when(c >= HOLD)
        def _():
            x2x(c - HOLD).wait_send()

        sx[lax.rem(c, HOLD)] = total(2)
        sd[lax.rem(c, 2), 0] = total(1)
        d2d(c, 0).start()
        base[c] += total(0)
        d2d(c, 1).wait_recv()
        sx[lax.rem(c, HOLD)] += rd[lax.rem(c, 2), 1]
        x2x(c).start()
        return 0

    lax.fori_loop(0, nc, chunk, 0)
    settle(nc - 1)
    for c in (nc - 2, nc - 1):
        for k in range(2):
            d2d(c, k).wait_send()

    for k in range(ns):
        wait(shared_in(k))
        w = min(wa, fs - k * wa)
        z = _dot(xa[...], wbuf[(n0 + k) % SLOTS, :, :2 * w])
        sb[:, k * wa:k * wa + w] = _silu_mul(z[:, :w], z[:, w:])
        if k == 0:
            start(shared_a)
        elif k == 1:
            start(shared_b)

    def add(z, lo):
        for c in range(z.shape[1] // BLK):
            base[lo // BLK + c] += z[:, c * BLK:(c + 1) * BLK]

    wait(shared_a)
    add(_dot(sb[:, :d], wbuf[slot_a]), 0)
    wait(shared_b)
    add(_dot(sb[:, :d], wbuf[slot_b, :, :tail]), wide)
    add(_dot(sb[:, d:], wbuf[slot_b, :rest, tail:]), 0)
    add(_dot(sb[:, d:], wbuf[slot_b, rest:2 * rest, tail:]), half)

    def put(c):
        cols = pl.ds(pl.multiple_of(c * BLK, BLK), BLK)
        return load(xa.at[:, cols], out_hbm.at[:, cols], osem.at[c])

    def finish(c, _):
        x2x(c).wait_recv()
        xa[:, pl.ds(pl.multiple_of(c * BLK, BLK), BLK)] = (base[c] + rx[c]).astype(BF16)
        put(c).start()
        return 0

    lax.fori_loop(0, nc, finish, 0)
    for c in range(nc - HOLD, nc):
        x2x(c).wait_send()

    def drain(c, _):
        put(c).wait()
        return 0

    lax.fori_loop(0, nc, drain, 0)


def solution(mesh):
    rows = P(('dp', 'ep'))
    rep = P()

    def local(h0, idx, slot, ln_attn, wq, wk, wv, wo, ln_ffn, ws1, ws3, ws2, ln_moe, wr, ue1, ue3, ue2):
        b, s, d = h0.shape
        top = idx.shape[-1]
        el, _, fe = ue1.shape
        fs = ws1.shape[1]
        t = b * s
        cap = CAP_FACTOR * t * top // (el * mesh.shape['ep'])
        nc = d // BLK
        wide = 2 * ((fe // 2 + HEAD - 1) // HEAD * HEAD)
        hbm = pl.BlockSpec(memory_space=pl.ANY)
        vmem = pl.BlockSpec(memory_space=pltpu.VMEM)
        dma = pltpu.SemaphoreType.DMA
        out = pl.pallas_call(
            functools.partial(_layer, el, cap, top),
            in_specs=[vmem] * 5 + [hbm] * 13,
            out_specs=hbm,
            out_shape=jax.ShapeDtypeStruct((t, d), BF16),
            scratch_shapes=[
                pltpu.VMEM((t, d), BF16), pltpu.VMEM((2, s, HEAD), F32), pltpu.VMEM((wr.shape[1], d), BF16),
                pltpu.VMEM((SLOTS, d, wide), BF16), pltpu.VMEM((el, 4 * cap, fe), BF16),
                pltpu.VMEM((4, t, d), BF16), pltpu.VMEM((t, d), BF16), pltpu.VMEM((t, fs), BF16),
                pltpu.VMEM((GROUP, 4 * cap, d), BF16), pltpu.VMEM((4, el * cap, BLK), BF16),
                pltpu.VMEM((4, 3 * t, el * cap), BF16), pltpu.VMEM((4, 8, t), jnp.int32),
                pltpu.VMEM((2, 2, t, BLK), F32), pltpu.VMEM((2, 2, t, BLK), F32),
                pltpu.VMEM((HOLD, t, BLK), F32), pltpu.VMEM((nc, t, BLK), F32), pltpu.VMEM((nc, t, BLK), F32),
                dma((3,)), dma((SLOTS, GROUP)), dma((nc,)), dma((2 * PIECES + 1,)), dma((2 * PIECES + 1,)), dma((3,)), dma((3,)),
                dma((2, 2)), dma((2, 2)), dma((HOLD,)), dma((nc,)),
            ],
            compiler_params=pltpu.CompilerParams(collective_id=0, has_side_effects=True, vmem_limit_bytes=67043328),
            name='layer',
        )(idx.reshape(t, 1, top).transpose(2, 1, 0), slot.reshape(t, 1, top).transpose(2, 1, 0), ln_attn, ln_ffn, ln_moe,
          h0.reshape(t, d), jnp.asarray(_tables(s)), wr.T, wq, wk, wv, wo, ws1, ws3, ws2, ue1, ue3, ue2)
        return out.reshape(b, s, d)

    specs = (rows, rows, rows) + (rep,) * 11 + (P('ep'), P('ep'), P('ep'))
    return jax.shard_map(local, mesh=mesh, in_specs=specs, out_specs=rows, check_vma=False)
```

```python
import functools

import jax
import jax.numpy as jnp
import numpy as np
from jax import lax
from jax.experimental import pallas as pl
from jax.experimental.pallas import tpu as pltpu
from jax.sharding import PartitionSpec as P

HEAD = 128
EPS = 1e-6
CAP_FACTOR = 2
BLK = 256
SLOTS = 4
GROUP = 4
PIECES = 4
HOLD = 4
EARLY = 2
MESH = pl.DeviceIdType.MESH
F32, BF16 = jnp.float32, jnp.bfloat16


def _dot(a, b):
    return jnp.dot(a, b, preferred_element_type=F32)


def _rms(x, w):
    xf = x.astype(F32)
    r = lax.rsqrt(jnp.mean(xf * xf, axis=-1, keepdims=True) + EPS)
    return (xf * r * w).astype(BF16)


def _silu_mul(h1, h3):
    return (h1 * jax.nn.sigmoid(h1) * h3).astype(BF16)


def _tables(s):
    half = HEAD // 2
    freq = np.float32(10000.0) ** (-np.arange(half, dtype=np.float32) / np.float32(half))
    ang = np.arange(s, dtype=np.float32)[:, None] * freq[None, :]
    c, sn = np.cos(ang), np.sin(ang)
    return np.stack([np.concatenate([c, c], axis=-1), np.concatenate([-sn, sn], axis=-1)]).astype(np.float32)


def _layer(el, cap, top, idx_ref, slot_ref, la_ref, lf_ref, lm_ref, h_hbm, tab_hbm, wr_hbm, wq, wk, wv, wo, ws1, ws3, ws2, ue1, ue3, ue2, out_hbm,
           h_ref, tab_ref, wr_ref, wbuf, he, ub, xa, sb, x4, ys, cm, pts, sd, rd, sx, rx, base,
           isem, wsem, osem, hs_sem, hr_sem, ps_sem, pr_sem, sd_sem, rd_sem, sx_sem, rx_sem):
    me = lax.axis_index('ep')
    dp = lax.axis_index('dp')
    core = (dp, me + 1 - 2 * lax.rem(me, 2))
    chip = (dp, lax.rem(me + 2, 4))
    t, d = h_ref.shape
    fe, fs = ue1.shape[2], ws1.shape[1]
    wide = wbuf.shape[2]
    wa = wide // 2
    widths = (wa, fe - wa)
    nc = d // BLK
    hw = wide // 3
    na = d // hw
    first = me * (el * cap)

    def load(src, dst, sem):
        return pltpu.make_async_copy(src, dst, sem)

    def send(src, dst, s, r, peer):
        return pltpu.make_async_remote_copy(src, dst, s, r, device_id=peer, device_id_type=MESH)

    def qkv(i, slot):
        cols = pl.ds(pl.multiple_of(i * hw, hw), hw)
        return [load(w.at[:, cols], wbuf.at[slot, :, k * hw:(k + 1) * hw], wsem.at[slot, k])
                for k, w in enumerate((wq, wk, wv))]

    wo_a = [load(wo.at[:, :wide], wbuf.at[na % SLOTS], wsem.at[na % SLOTS, 0])]
    wo_b = [load(wo.at[:, wide:], wbuf.at[(na + 1) % SLOTS, :, :d - wide], wsem.at[(na + 1) % SLOTS, 0])]

    def unit(e, h, slot):
        w, lo = widths[h], h * wa
        return [load(ue.at[e, :, lo:lo + w], wbuf.at[slot, :, k * w:(k + 1) * w], wsem.at[slot, k])
                for k, ue in enumerate((ue1, ue3))]

    def pieces(c, i, slot):
        cols = pl.ds(pl.multiple_of(c * BLK, BLK), BLK)
        return [load(ue2.at[GROUP * i + k, :, cols], wbuf.at[slot, :fe, k * BLK:(k + 1) * BLK], wsem.at[slot, k])
                for k in range(GROUP)]

    def shared_in(k):
        lo, w = k * wa, min(wa, fs - k * wa)
        n = (na + 2 + k) % SLOTS
        return [load(ws.at[:, lo:lo + w], wbuf.at[n, :, i * w:(i + 1) * w], wsem.at[n, i])
                for i, ws in enumerate((ws1, ws3))]

    ns = -(-fs // wa)
    up0 = na + 2 + EARLY
    down0 = up0 + 2 * el
    n0 = down0 + nc * (el // GROUP)
    slot_a, slot_b = (n0 + ns - EARLY) % SLOTS, (n0 + ns - EARLY + 1) % SLOTS
    rest, tail = fs - d, d - wide
    half = wide - tail
    shared_a = [load(ws2.at[:d, :wide], wbuf.at[slot_a], wsem.at[slot_a, 0])]
    shared_b = [load(ws2.at[:d, wide:], wbuf.at[slot_b, :, :tail], wsem.at[slot_b, 0]),
                load(ws2.at[d:, :half], wbuf.at[slot_b, :rest, tail:], wsem.at[slot_b, 1]),
                load(ws2.at[d:, half:], wbuf.at[slot_b, rest:2 * rest, tail:], wsem.at[slot_b, 2])]

    def start(copies):
        for cp in copies:
            cp.start()

    def wait(copies):
        for cp in copies:
            cp.wait()

    own = [load(h_hbm, h_ref, isem.at[0]), load(tab_hbm, tab_ref, isem.at[1]), load(wr_hbm, wr_ref, isem.at[2])]
    start(own)
    for n in range(SLOTS):
        start(qkv(n, n))
    pts[0] = jnp.concatenate([idx_ref[j] * cap + slot_ref[j] for j in range(top)]
                             + [jnp.full((pts.shape[1] - top, t), -1, jnp.int32)], axis=0)
    ln_a, ln_f, ln_m = (r[...].astype(F32).reshape(1, d) for r in (la_ref, lf_ref, lm_ref))

    barrier = pltpu.get_barrier_semaphore()
    for peer in (core, chip):
        pl.semaphore_signal(barrier, inc=1, device_id=peer, device_id_type=MESH)
    pl.semaphore_wait(barrier, 2)

    rows = t // PIECES
    part = [pl.ds(q * rows, rows) for q in range(PIECES)]
    far = [send(h_hbm.at[part[q]], ub.at[2, part[q]], hs_sem.at[q], hr_sem.at[q], chip) for q in range(PIECES)]
    near = send(h_hbm, ub.at[1], hs_sem.at[PIECES], hr_sem.at[PIECES], core)
    onward = [send(ub.at[2, part[q]], ub.at[3, part[q]], hs_sem.at[PIECES + 1 + q], hr_sem.at[PIECES + 1 + q], core)
              for q in range(PIECES)]
    pfar = send(pts.at[0], pts.at[2], ps_sem.at[0], pr_sem.at[0], chip)
    pnear = send(pts.at[0], pts.at[1], ps_sem.at[1], pr_sem.at[1], core)
    ponward = send(pts.at[2], pts.at[3], ps_sem.at[2], pr_sem.at[2], core)
    start(far)
    near.start()
    wait(own)

    xa[...] = _rms(h_ref[...], ln_a)
    ub[0] = _rms(h_ref[...], ln_m)
    pfar.start()
    pnear.start()

    def heads(i, _):
        slot = lax.rem(i, SLOTS)
        wait(qkv(i, slot))
        z = _dot(xa[...], wbuf[slot])

        for k, nxt in enumerate((wo_a, wo_b, shared_in(0), shared_in(1))):
            @pl.when(i == k)
            def _():
                start(nxt)

        c, s = tab_ref[0], tab_ref[1]
        ok = lax.broadcasted_iota(jnp.int32, (t, t), 0) >= lax.broadcasted_iota(jnp.int32, (t, t), 1)
        outs = []
        for j in range(hw // HEAD):
            qj, kj, vj = (z[:, m * hw + j * HEAD:m * hw + (j + 1) * HEAD] for m in range(3))
            qj = (qj * c + pltpu.roll(qj, HEAD // 2, 1) * s).astype(BF16)
            kj = (kj * c + pltpu.roll(kj, HEAD // 2, 1) * s).astype(BF16)
            sc = lax.dot_general(qj, kj, (((1,), (1,)), ((), ())), preferred_element_type=F32) * HEAD ** -0.5
            sc = jnp.where(ok, sc, -1e30)
            e = jnp.exp(sc - jnp.max(sc, axis=-1, keepdims=True))
            p = (e / jnp.sum(e, axis=-1, keepdims=True)).astype(BF16)
            outs.append(_dot(p, vj.astype(BF16)).astype(BF16))
        sb[:, pl.ds(pl.multiple_of(i * hw, hw), hw)] = jnp.concatenate(outs, axis=-1)
        return 0

    lax.fori_loop(0, na, heads, 0)

    def pass_on(q):
        far[q].wait_recv()
        onward[q].start()

    pfar.wait_recv()
    ponward.start()
    pass_on(0)
    pass_on(1)

    def residual(z, lo):
        a = (h_ref[:, lo:lo + z.shape[1]].astype(F32) + z).astype(BF16)
        xa[:, lo:lo + z.shape[1]] = a
        for c in range(z.shape[1] // BLK):
            base[lo // BLK + c] = a[:, c * BLK:(c + 1) * BLK].astype(F32)

    wait(wo_a)
    residual(_dot(sb[:, :d], wbuf[na % SLOTS]), 0)
    start(unit(0, 0, up0 % SLOTS))
    wait(wo_b)
    residual(_dot(sb[:, :d], wbuf[(na + 1) % SLOTS, :, :d - wide]), wide)
    start(unit(0, 1, (up0 + 1) % SLOTS))
    xa[...] = _rms(xa[...], ln_f)

    def shared_up(k):
        wait(shared_in(k))
        w = min(wa, fs - k * wa)
        z = _dot(xa[...], wbuf[(na + 2 + k) % SLOTS, :, :2 * w])
        sb[:, k * wa:k * wa + w] = _silu_mul(z[:, :w], z[:, w:])

    shared_up(0)
    start(unit(1, 0, (up0 + 2) % SLOTS))
    pass_on(2)
    shared_up(1)
    start(unit(1, 1, (up0 + 3) % SLOTS))
    off = up0 % SLOTS

    def weigh(k):
        pos = jnp.concatenate([pts[k].astype(F32), jnp.zeros((HEAD - pts.shape[1], t), F32)], axis=0).T
        lg = lax.dot_general(ub[k], wr_ref[...], (((1,), (1,)), ((), ())), preferred_element_type=F32)
        lo = lax.broadcasted_iota(jnp.int32, lg.shape, 1).astype(F32) * cap
        picks = []
        for j in range(top):
            off = pos[:, j:j + 1] - lo
            hit = jnp.logical_and(off >= 0, off < cap)
            picks.append(jnp.sum(jnp.where(hit, lg, 0.0), axis=-1, keepdims=True))
        big = functools.reduce(jnp.maximum, picks)
        ex = [jnp.exp(p - big) for p in picks]
        tot = functools.reduce(jnp.add, ex)
        r = (lax.broadcasted_iota(jnp.int32, (t, el * cap), 1) + first).astype(F32)
        c = jnp.zeros(r.shape, F32)
        for j in range(top):
            c += jnp.where(pos[:, j:j + 1] == r, ex[j] / tot, 0.0)
        hi = c.astype(BF16)
        c -= hi.astype(F32)
        mid = c.astype(BF16)
        cm[k, :t] = hi
        cm[k, t:2 * t] = mid
        cm[k, 2 * t:] = (c - mid.astype(F32)).astype(BF16)

    near.wait_recv()
    pnear.wait_recv()
    ub[1] = _rms(ub[1], ln_m)

    pass_on(3)
    for cp in onward:
        cp.wait_send()
    ub[2] = _rms(ub[2], ln_m)
    for cp in onward:
        cp.wait_recv()
    ub[3] = _rms(ub[3], ln_m)
    ponward.wait()
    pfar.wait_send()
    pnear.wait_send()
    near.wait_send()
    for cp in far:
        cp.wait_send()

    def group(g, last):
        weigh(g)
        for k in range(4):
            r = lax.broadcasted_iota(jnp.int32, (GROUP * cap, t), 0) + (first + g * (GROUP * cap))
            hit = pts[k, 0:1, :] == r
            for j in range(1, top):
                hit = jnp.logical_or(hit, pts[k, j:j + 1, :] == r)
            x = _dot(hit.astype(F32).astype(BF16), ub[k]).astype(BF16)
            for j in range(GROUP):
                x4[j, k * cap:(k + 1) * cap, :] = x[j * cap:(j + 1) * cap]

        def ffn_in(j, _):
            e = g * GROUP + j
            for h in range(2):
                slot = lax.rem(2 * e + h + off, SLOTS)
                w = widths[h]
                wait(unit(e, h, slot))
                z = _dot(x4[j], wbuf[slot, :, :2 * w])
                he[e, :, h * wa:h * wa + w] = _silu_mul(z[:, :w], z[:, w:])

                @pl.when(e + 2 < el)
                def _():
                    start(unit(e + 2, h, slot))

                @pl.when(e + 2 >= el)
                def _():
                    start(pieces(0, 2 * (e + 2 - el) + h, slot))
            return 0

        lax.fori_loop(0, GROUP, ffn_in, 0)
        return last

    lax.fori_loop(0, el // GROUP, group, 0)

    def d2d(c, k):
        p = lax.rem(c, 2)
        return send(sd.at[p, k], rd.at[p, k], sd_sem.at[p, k], rd_sem.at[p, k], core)

    def x2x(c):
        p = lax.rem(c, HOLD)
        return send(sx.at[p], rx.at[c], sx_sem.at[p], rx_sem.at[c], chip)

    def settle(c):
        d2d(c, 0).wait_recv()
        base[c] += rd[lax.rem(c, 2), 0]

    def chunk(c, _):
        def duo(m, _):
            steps = [(2 * m + q, lax.rem(2 * m + q + down0, SLOTS)) for q in range(2)]
            for i, slot in steps:
                wait(pieces(c, i, slot))
            for i, slot in steps:
                for k in range(GROUP):
                    e = GROUP * i + k
                    y = _dot(he[e], wbuf[slot, :fe, k * BLK:(k + 1) * BLK]).astype(BF16)
                    for b in range(4):
                        ys[b, pl.ds(pl.multiple_of(e * cap, cap), cap), :] = y[b * cap:(b + 1) * cap]

            @pl.when(c + 1 < nc)
            def _():
                for i, slot in steps:
                    start(pieces(c + 1, i, slot))

            for k, late in enumerate((shared_in(2) + shared_in(3), shared_a + shared_b)):
                @pl.when(jnp.logical_and(c + 1 == nc, m == k))
                def _():
                    start(late)
            return 0

        lax.fori_loop(0, el // GROUP // 2, duo, 0)

        @pl.when(c >= 2)
        def _():
            for k in range(2):
                d2d(c - 2, k).wait_send()

        @pl.when(c >= 1)
        def _():
            settle(c - 1)

        def total(k):
            z = _dot(cm[k], ys[k])
            return z[:t] + z[t:2 * t] + z[2 * t:]

        sd[lax.rem(c, 2), 1] = total(3)
        d2d(c, 1).start()

        @pl.when(c >= HOLD)
        def _():
            x2x(c - HOLD).wait_send()

        sx[lax.rem(c, HOLD)] = total(2)
        sd[lax.rem(c, 2), 0] = total(1)
        d2d(c, 0).start()
        base[c] += total(0)
        d2d(c, 1).wait_recv()
        sx[lax.rem(c, HOLD)] += rd[lax.rem(c, 2), 1]
        x2x(c).start()
        return 0

    lax.fori_loop(0, nc, chunk, 0)
    settle(nc - 1)
    for c in (nc - 2, nc - 1):
        for k in range(2):
            d2d(c, k).wait_send()

    for k in range(EARLY, ns):
        shared_up(k)

    def add(z, lo):
        for c in range(z.shape[1] // BLK):
            base[lo // BLK + c] += z[:, c * BLK:(c + 1) * BLK]

    wait(shared_a)
    add(_dot(sb[:, :d], wbuf[slot_a]), 0)
    wait(shared_b)
    add(_dot(sb[:, :d], wbuf[slot_b, :, :tail]), wide)
    add(_dot(sb[:, d:], wbuf[slot_b, :rest, tail:]), 0)
    add(_dot(sb[:, d:], wbuf[slot_b, rest:2 * rest, tail:]), half)

    def put(c):
        cols = pl.ds(pl.multiple_of(c * BLK, BLK), BLK)
        return load(base.at[c], out_hbm.at[:, cols], osem.at[c])

    def finish(c, _):
        x2x(c).wait_recv()
        base[c] += rx[c]
        put(c).start()
        return 0

    lax.fori_loop(0, nc, finish, 0)
    for c in range(nc - HOLD, nc):
        x2x(c).wait_send()

    def drain(c, _):
        put(c).wait()
        return 0

    lax.fori_loop(0, nc, drain, 0)


def solution(mesh):
    rows = P(('dp', 'ep'))
    rep = P()

    def local(h0, idx, slot, ln_attn, wq, wk, wv, wo, ln_ffn, ws1, ws3, ws2, ln_moe, wr, ue1, ue3, ue2):
        b, s, d = h0.shape
        top = idx.shape[-1]
        el, _, fe = ue1.shape
        fs = ws1.shape[1]
        t = b * s
        cap = CAP_FACTOR * t * top // (el * mesh.shape['ep'])
        nc = d // BLK
        wide = 2 * ((fe // 2 + HEAD - 1) // HEAD * HEAD)
        hbm = pl.BlockSpec(memory_space=pl.ANY)
        vmem = pl.BlockSpec(memory_space=pltpu.VMEM)
        dma = pltpu.SemaphoreType.DMA
        out = pl.pallas_call(
            functools.partial(_layer, el, cap, top),
            in_specs=[vmem] * 5 + [hbm] * 13,
            out_specs=hbm,
            out_shape=jax.ShapeDtypeStruct((t, d), F32),
            scratch_shapes=[
                pltpu.VMEM((t, d), BF16), pltpu.VMEM((2, s, HEAD), F32), pltpu.VMEM((wr.shape[1], d), BF16),
                pltpu.VMEM((SLOTS, d, wide), BF16), pltpu.VMEM((el, 4 * cap, fe), BF16),
                pltpu.VMEM((4, t, d), BF16), pltpu.VMEM((t, d), BF16), pltpu.VMEM((t, fs), BF16),
                pltpu.VMEM((GROUP, 4 * cap, d), BF16), pltpu.VMEM((4, el * cap, BLK), BF16),
                pltpu.VMEM((4, 3 * t, el * cap), BF16), pltpu.VMEM((4, 8, t), jnp.int32),
                pltpu.VMEM((2, 2, t, BLK), F32), pltpu.VMEM((2, 2, t, BLK), F32),
                pltpu.VMEM((HOLD, t, BLK), F32), pltpu.VMEM((nc, t, BLK), F32), pltpu.VMEM((nc, t, BLK), F32),
                dma((3,)), dma((SLOTS, GROUP)), dma((nc,)), dma((2 * PIECES + 1,)), dma((2 * PIECES + 1,)), dma((3,)), dma((3,)),
                dma((2, 2)), dma((2, 2)), dma((HOLD,)), dma((nc,)),
            ],
            compiler_params=pltpu.CompilerParams(collective_id=0, has_side_effects=True, vmem_limit_bytes=67043328),
            name='layer',
        )(idx.reshape(t, 1, top).transpose(2, 1, 0), slot.reshape(t, 1, top).transpose(2, 1, 0), ln_attn, ln_ffn, ln_moe,
          h0.reshape(t, d), jnp.asarray(_tables(s)), wr.T, wq, wk, wv, wo, ws1, ws3, ws2, ue1, ue3, ue2)
        return out.astype(BF16).reshape(b, s, d)

    specs = (rows, rows, rows) + (rep,) * 11 + (P('ep'), P('ep'), P('ep'))
    return jax.shard_map(local, mesh=mesh, in_specs=specs, out_specs=rows, check_vma=False)
```
